32 devices in a mesh: crops: 2 (over y), rows: 4 (over z), chan: 2 (over x), sub: 2 (over core).
Axes of the slice: x: 2, y: 2, z: 4, core: 2. Of those that a mesh axis runs over, the one named last changes fastest.
Arguments:
- pair: bfloat16 [64, 32, 128], P(('crops', 'rows', 'sub')), parts along dimension 0, may hold values from -6 to 6
- residue_mask: int32 [64], P('crops'), parts along dimension 0, may hold values from 0 to 1, as said below
- in_gain: float32 [2, 128], replicated, may hold values from 0.1 to 1.9
- in_bias: float32 [2, 128], replicated, may hold values from -3 to 3
- projections: bfloat16 [2, 4, 128, 128], P(None, None, None, 'chan'), may hold values from -0.5 to 0.5
- gate_weight: bfloat16 [2, 128, 128], replicated, may hold values from -0.5 to 0.5
- out_gain: float32 [2, 128], replicated, may hold values from 0.1 to 1.9
- out_bias: float32 [2, 128], replicated, may hold values from -3 to 3
- out_weight: bfloat16 [2, 128, 128], replicated, may hold values from -0.5 to 0.5
Outputs:
- pair_out: bfloat16 [64, 32, 128], P(('crops', 'rows', 'sub'), 'chan'), parts along dimension 0
The draws below stay inside these ranges and needn't reach their ends.
There are 2 independent parts, one for each index of `crops`. The reference program is written for one: setup_inputs(seed, part) draws one part's arguments, and reference() takes and returns one part's arrays. A program takes and returns all parts, laid end to end along the dimension named above; an argument that names none is the same for every part. Nothing has to cross between parts.
Inputs may be any that keep to these rules, and one draw needn't show every extreme that they name: `residue_mask`: residue 0 is always present and residue 32 - 1 is always a gap or padding.
All inputs are finite; a program needn't handle non-finite values.
Results may differ from the reference program's by a relative error of at most 0.012.
Values may be sent and summed in bfloat16 or wider, within the bound.
No kernel may reach another device: no remote copies, remote signals or barrier semaphores. Data moves between devices by JAX's collectives and lax.ppermute only.
A program may use at most 64 MiB of HBM per device.

```python
import jax
import jax.numpy as jnp
from jax import lax

C = 128
H = 128
N = 32


def draw_residue_mask(key, part):
    levels = jax.random.randint(jax.random.fold_in(key, 7), (N,), 0, 4)
    present = (levels != 0).astype(jnp.int32)
    positions = jnp.arange(N)
    present = jnp.where(positions == 0, 1, present)
    present = jnp.where(positions == N - 1, 0, present)
    return present.astype(jnp.int32)


def shard_levels(stream_key, shape, shards, smallest, largest):
    def one(dim, blocks):
        steps = jax.random.uniform(jax.random.fold_in(jax.random.fold_in(stream_key, 6), dim), (blocks,), jnp.float32, smallest / len(shards), largest / len(shards))
        return jnp.repeat(jnp.exp(steps), shape[dim] // blocks).reshape((-1,) + (1,) * (len(shape) - dim - 1))

    loudness = one(*shards[0])
    for cut in shards[1:]:
        loudness = loudness * one(*cut)
    return loudness


def normal_values(rng, shape, scale, most, pieces=(), dtype=jnp.bfloat16):
    result = jax.random.normal(rng, shape, jnp.float32) * scale
    if len(pieces) > 0:
        result = shard_levels(rng, shape, pieces, -0.22, 0.18) * result
    return jnp.clip(result, min=-most, max=most).astype(dtype)


def setup_inputs(seed: int = 0, part: int = 0) -> dict:
    key_of = jax.random.split(jax.random.key(seed), 10)
    part_splits = jax.random.split(jax.random.fold_in(key_of[9], part), 10)
    return {
        "pair": normal_values(part_splits[0], (N, N, C), 1.0, 6.0, ((0, 8),)),
        "residue_mask": draw_residue_mask(jax.random.fold_in(jax.random.fold_in(key_of[9], part), 71), part),
        "in_gain": jnp.clip(1.0 + 0.18 * jax.random.normal(key_of[2], (2, C), jnp.float32), 0.1, 1.9),
        "in_bias": normal_values(key_of[3], (2, C), 0.5, 3.0, (), jnp.float32),
        "projections": normal_values(key_of[4], (2, 4, C, H), C ** -0.5, 0.5, ((3, 2),)),
        "gate_weight": normal_values(key_of[5], (2, C, C), C ** -0.5, 0.5),
        "out_gain": jnp.clip(1.0 + 0.18 * jax.random.normal(key_of[6], (2, H), jnp.float32), 0.1, 1.9),
        "out_bias": normal_values(key_of[7], (2, H), 0.5, 3.0, (), jnp.float32),
        "out_weight": normal_values(key_of[8], (2, H, C), H ** -0.5, 0.5),
    }


epsilon = 1e-05

def normalize(values, reduce_axis):
    centre = lax.optimization_barrier(jnp.mean(values, axis=reduce_axis, keepdims=True))
    centred = values - centre
    spread = lax.optimization_barrier(jnp.mean(centred * centred, axis=reduce_axis, keepdims=True))
    return centred * lax.rsqrt(spread + epsilon)

def update_layer(pair, pair_mask, layer_index, incoming, in_gain, in_bias, projections, gate_weight, out_gain, out_bias, out_weight):
    pair_float = pair.astype(jnp.float32)
    normed = (normalize(pair_float, 2) * in_gain[layer_index] + in_bias[layer_index]).astype(jnp.bfloat16)
    projected = jnp.einsum('ikc,qch->qikh', normed.astype(jnp.float32), projections[layer_index].astype(jnp.float32), precision=lax.Precision.HIGHEST)
    left_edges = (jax.nn.sigmoid(projected[0]) * projected[1] * pair_mask).astype(jnp.bfloat16)
    right_edges = (jax.nn.sigmoid(projected[2]) * projected[3] * pair_mask).astype(jnp.bfloat16)
    if incoming:
        triangle = jnp.einsum('kih,kjh->ijh', left_edges.astype(jnp.float32), right_edges.astype(jnp.float32), precision=lax.Precision.HIGHEST)
    else:
        triangle = jnp.einsum('ikh,jkh->ijh', left_edges.astype(jnp.float32), right_edges.astype(jnp.float32), precision=lax.Precision.HIGHEST)
    triangle = triangle.astype(jnp.bfloat16)
    scaled = (normalize(triangle.astype(jnp.float32), 2) * out_gain[layer_index] + out_bias[layer_index]).astype(jnp.bfloat16)
    update = jnp.einsum('ijh,hc->ijc', scaled.astype(jnp.float32), out_weight[layer_index].astype(jnp.float32), precision=lax.Precision.HIGHEST)
    gating = jax.nn.sigmoid(jnp.einsum('ijc,cd->ijd', normed.astype(jnp.float32), gate_weight[layer_index].astype(jnp.float32), precision=lax.Precision.HIGHEST))
    return (pair_float + gating * update).astype(jnp.bfloat16)

def reference(pair, residue_mask, in_gain, in_bias, projections, gate_weight, out_gain, out_bias, out_weight):
    mask_float = residue_mask.astype(jnp.float32)
    pair_mask = mask_float[:, None, None] * mask_float[None, :, None]
    layer_one = update_layer(pair, pair_mask, 0, False, in_gain, in_bias, projections, gate_weight, out_gain, out_bias, out_weight)
    return update_layer(layer_one, pair_mask, 1, True, in_gain, in_bias, projections, gate_weight, out_gain, out_bias, out_weight)
```

```python
import functools

import jax
import jax.numpy as jnp
from jax import lax
from jax.experimental import pallas as pl
from jax.experimental.pallas import tpu as pltpu
from jax.sharding import PartitionSpec as P

epsilon = 1e-05


GATHER_LIMIT = 1 << 20


def normalize(values, reduce_axis):
    centre = jnp.mean(values, axis=reduce_axis, keepdims=True)
    centred = values - centre
    spread = jnp.mean(centred * centred, axis=reduce_axis, keepdims=True)
    return centred * lax.rsqrt(spread + epsilon)


def shards(
    pair, residue_mask, in_gain, in_bias, projections, gate_weight, out_gain, out_bias, out_weight
):
    rows_block = pair.shape[0]
    length = pair.shape[1]
    chan_count = lax.axis_size("chan")
    chan_index = lax.axis_index("chan")
    quarter = length // chan_count
    row_start = lax.axis_index(("rows", "sub")) * rows_block
    mask_float = residue_mask.astype(jnp.float32)
    own_mask = lax.dynamic_slice_in_dim(mask_float, row_start, rows_block)
    pair_mask = own_mask[None, :, None] * mask_float[None, None, :]

    def project(full_rows, layer_index):
        normed = (
            normalize(full_rows.astype(jnp.float32), 2) * in_gain[layer_index]
            + in_bias[layer_index]
        ).astype(jnp.bfloat16)
        projected = jnp.einsum(
            "ikc,qch->qhik", normed, projections[layer_index], preferred_element_type=jnp.float32
        )
        left_edges = (jax.nn.sigmoid(projected[0]) * projected[1] * pair_mask).astype(jnp.bfloat16)
        right_edges = (jax.nn.sigmoid(projected[2]) * projected[3] * pair_mask).astype(jnp.bfloat16)
        return (normed, left_edges, right_edges)

    def finish(triangle, normed, residual, layer_index):
        gathered = lax.all_to_all(triangle, "chan", split_axis=2, concat_axis=0, tiled=True)
        whole_float = gathered.astype(jnp.float32)
        scaled = (
            normalize(whole_float, 0) * out_gain[layer_index][:, None, None]
            + out_bias[layer_index][:, None, None]
        ).astype(jnp.bfloat16)
        update = jnp.einsum(
            "hij,hc->ijc", scaled, out_weight[layer_index], preferred_element_type=jnp.float32
        )
        normed_part = lax.dynamic_slice_in_dim(normed, chan_index * quarter, quarter, 1)
        gating = jax.nn.sigmoid(
            jnp.einsum(
                "ijc,cd->ijd",
                normed_part,
                gate_weight[layer_index],
                preferred_element_type=jnp.float32,
            )
        )
        return (residual.astype(jnp.float32) + gating * update).astype(jnp.bfloat16)

    normed, left_edges, right_edges = project(pair, 0)
    triangle = jnp.einsum(
        "hik,hjk->hij",
        left_edges,
        lax.all_gather(right_edges, ("rows", "sub"), axis=1, tiled=True),
        preferred_element_type=jnp.float32,
    ).astype(jnp.bfloat16)
    own_quarter = lax.dynamic_slice_in_dim(pair, chan_index * quarter, quarter, 1)
    layer_one = finish(triangle, normed, own_quarter, 0)
    full_rows = lax.all_gather(layer_one, "chan", axis=1, tiled=True)
    normed, left_edges, right_edges = project(full_rows, 1)
    left_cols, right_cols = (
        lax.all_to_all(left_edges, ("rows", "sub"), split_axis=2, concat_axis=1, tiled=True),
        lax.all_to_all(right_edges, ("rows", "sub"), split_axis=2, concat_axis=1, tiled=True),
    )
    triangle = jnp.einsum(
        "hki,hkj->hij",
        left_cols,
        lax.all_gather(right_cols, ("rows", "sub"), axis=2, tiled=True),
        preferred_element_type=jnp.float32,
    )
    return finish(triangle.astype(jnp.bfloat16), normed, layer_one, 1)


def swap(value, axis, step):
    count = lax.axis_size(axis)
    return lax.ppermute(value, axis, [(i, i ^ step) for i in range(count)])


def mm(a, b):
    return jnp.dot(a, b, preferred_element_type=jnp.float32)


def mmt(a, b):
    return lax.dot_general(a, b, (((1,), (1,)), ((), ())), preferred_element_type=jnp.float32)


def layer_norm(values, gain, bias, average):
    centred = values.astype(jnp.float32) - mm(values, average)
    square = centred * centred
    high = square.astype(jnp.bfloat16)
    low = (square - high.astype(jnp.float32)).astype(jnp.bfloat16)
    spread = mm(high, average) + mm(low, average)
    return (centred * lax.rsqrt(spread + epsilon) * gain + bias).astype(jnp.bfloat16)


def gated(gate, value):
    half = 0.5 * value
    return half * jnp.tanh(0.5 * gate) + half


def crop_kernel(steps, counts, *refs):
    rows_count, chan_count, sub_count = counts
    blocks = [refs[i] for i in range(len(steps))]
    weights = [refs[len(steps) + i] for i in range(chan_count)]
    (mask_ref, ig_ref, ib_ref, gw_ref, og_ref, ob_ref, ow_ref, out_ref,
     w_ref, normed_ref, left_ref, right_ref, turned_ref, tri_ref, z_ref, l1_ref, r1_ref) = refs[len(steps) + chan_count:]
    row = lax.axis_index("rows")
    chan = lax.axis_index("chan")
    sub = lax.axis_index("sub")
    own = row * sub_count + sub
    size, length, c = blocks[0].shape
    h = ow_ref.shape[1]
    quarter = length // chan_count
    part = h // chan_count
    area = size * length
    average = jnp.full((c, c), 1.0 / c, jnp.bfloat16)

    for i in range(chan_count):
        at = pl.multiple_of((chan ^ i) * part, part)
        w_ref[:, :, pl.ds(at, part), :] = weights[i][...]

    mask = mask_ref[...]

    for (rs, ss), block in zip(steps, blocks):
        b = (row ^ rs) * sub_count + (sub ^ ss)
        x = block[...].reshape(area, c)
        normed = layer_norm(x, ig_ref[0:1], ib_ref[0:1], average)
        normed_ref[pl.ds(b * size, size)] = normed.reshape(size, length, c)
        z_ref[pl.ds(b * size, size)] = x.astype(jnp.float32).reshape(size, length, c)
        both = mask_ref[pl.ds(b * size, size)][:, None, :] * mask[None]
        lg, lv, rg, rv = [mmt(normed, w_ref[0, q]).reshape(size, length, h) for q in range(4)]
        left_ref[pl.ds(b * size, size)] = gated(lg, lv) * both
        right_ref[pl.ds(b * size, size)] = gated(rg, rv) * both

    turned_ref[...] = jnp.swapaxes(right_ref[...], 0, 1)

    group = 8
    def outer(g, carry):
        k0 = g * group
        def inner(m, acc):
            r = turned_ref[m]
            return tuple(a + left_ref[k0 + i, pl.ds(m, 1), :] * r for i, a in enumerate(acc))
        acc = lax.fori_loop(0, length, inner, tuple(jnp.zeros((length, h), jnp.float32) for _ in range(group)), unroll=4)
        for i, a in enumerate(acc):
            tri_ref[k0 + i] = a.astype(jnp.bfloat16)
        return carry
    lax.fori_loop(0, length // group, outer, 0)

    def update(tri, normed, residual, layer):
        scaled = layer_norm(tri, og_ref[layer:layer + 1], ob_ref[layer:layer + 1], average)
        return residual + gated(mm(normed, gw_ref[layer]), mm(scaled, ow_ref[layer]))

    for b in range(length // size):
        at = slice(b * size, (b + 1) * size)
        z = update(tri_ref[at].reshape(area, h), normed_ref[at].reshape(area, c), z_ref[at].reshape(area, c), 0)
        z_ref[at] = z.astype(jnp.bfloat16).astype(jnp.float32).reshape(size, length, c)

    tile = 8
    i_tile = pl.multiple_of(own * size // tile * tile, tile)
    j_at = pl.multiple_of(chan * quarter, quarter)

    zi = z_ref[:, pl.ds(i_tile, tile), :].reshape(length * tile, c).astype(jnp.bfloat16)
    ni = layer_norm(zi, ig_ref[1:2], ib_ref[1:2], average)
    mi = (mask[:, None, :] * mask_ref[pl.ds(i_tile, tile)][None])
    l1_ref[...] = gated(mmt(ni, w_ref[1, 0]), mmt(ni, w_ref[1, 1])).reshape(length, tile, h) * mi
    zj = z_ref[:, pl.ds(j_at, quarter), :].reshape(length * quarter, c).astype(jnp.bfloat16)
    nj = layer_norm(zj, ig_ref[1:2], ib_ref[1:2], average)
    mj = (mask[:, None, :] * mask_ref[pl.ds(j_at, quarter)][None])
    r1_ref[...] = gated(mmt(nj, w_ref[1, 2]), mmt(nj, w_ref[1, 3])).reshape(length, quarter, h) * mj
    normed_ref[:, 0:quarter, :] = nj.reshape(length, quarter, c)

    first = own * size - i_tile
    def inner1(k, acc):
        r = r1_ref[k]
        return tuple(a + l1_ref[k, pl.ds(first + i, 1), :] * r for i, a in enumerate(acc))
    acc = lax.fori_loop(0, length, inner1, tuple(jnp.zeros((quarter, h), jnp.float32) for _ in range(size)), unroll=4)
    tri = jnp.concatenate(acc, 0).astype(jnp.bfloat16)
    mine = pl.ds(own * size, size)
    z = update(
        tri,
        normed_ref[mine, 0:quarter, :].reshape(size * quarter, c),
        z_ref[mine, pl.ds(j_at, quarter), :].reshape(size * quarter, c),
        1,
    )
    out_ref[...] = z.astype(jnp.bfloat16).reshape(size, quarter, c)


def gathered(
    pair, residue_mask, in_gain, in_bias, projections, gate_weight, out_gain, out_bias, out_weight
):
    rows_count, chan_count, sub_count = (lax.axis_size(a) for a in ("rows", "chan", "sub"))
    size, length, c = pair.shape
    h = out_weight.shape[1]
    turned = jnp.swapaxes(projections, 2, 3)
    weights = [turned] + [swap(turned, "chan", i) for i in range(1, chan_count)]
    steps, blocks = [(0, 0)], [pair]
    for rs in reversed(range(1, rows_count)):
        steps.append((rs, 0))
        blocks.append(swap(pair, "rows", rs))
    for ss in range(1, sub_count):
        for (rs, _), block in zip(steps[:rows_count], blocks[:rows_count]):
            steps.append((rs, ss))
            blocks.append(swap(block, "sub", ss))
    mask = jnp.broadcast_to(residue_mask.astype(jnp.float32)[:, None], (length, h))
    operands = [*blocks, *weights, mask, in_gain, in_bias, gate_weight, out_gain, out_bias, out_weight]
    vmem = pl.BlockSpec(memory_space=pltpu.VMEM)
    return pl.pallas_call(
        functools.partial(crop_kernel, tuple(steps), (rows_count, chan_count, sub_count)),
        out_shape=jax.ShapeDtypeStruct((size, length // chan_count, c), jnp.bfloat16),
        in_specs=[vmem] * len(operands),
        out_specs=vmem,
        scratch_shapes=[
            pltpu.VMEM((2, 4, h, c), jnp.bfloat16),
            pltpu.VMEM((length, length, c), jnp.bfloat16),
            pltpu.VMEM((length, length, h), jnp.float32),
            pltpu.VMEM((length, length, h), jnp.float32),
            pltpu.VMEM((length, length, h), jnp.float32),
            pltpu.VMEM((length, length, h), jnp.bfloat16),
            pltpu.VMEM((length, length, c), jnp.float32),
            pltpu.VMEM((length, 8, h), jnp.float32),
            pltpu.VMEM((length, length // chan_count, h), jnp.float32),
        ],
    )(*operands)


def power_of_two(n):
    return n & (n - 1) == 0


def solution(mesh):
    def body(pair, *rest):
        small = 2 * pair.shape[1] * pair.shape[1] * pair.shape[2] <= GATHER_LIMIT
        even = all(power_of_two(mesh.shape[a]) for a in ("rows", "chan", "sub"))
        return (gathered if small and even else shards)(pair, *rest)

    placed = (
        P(("crops", "rows", "sub"), None, None),
        P("crops"),
        P(),
        P(),
        P(None, None, None, "chan"),
        P(),
        P(),
        P(),
        P(),
    )
    return jax.shard_map(
        body,
        mesh=mesh,
        in_specs=placed,
        out_specs=P(("crops", "rows", "sub"), "chan", None),
        check_vma=False,
    )
```

```python
import functools

import jax
import jax.numpy as jnp
from jax import lax
from jax.experimental import pallas as pl
from jax.experimental.pallas import tpu as pltpu
from jax.sharding import PartitionSpec as P


epsilon = 1e-05


GATHER_LIMIT = 1 << 20


def normalize(values, reduce_axis):
    centre = jnp.mean(values, axis=reduce_axis, keepdims=True)
    centred = values - centre
    spread = jnp.mean(centred * centred, axis=reduce_axis, keepdims=True)
    return centred * lax.rsqrt(spread + epsilon)


def shards(
    pair, residue_mask, in_gain, in_bias, projections, gate_weight, out_gain, out_bias, out_weight
):
    rows_block = pair.shape[0]
    length = pair.shape[1]
    chan_count = lax.axis_size("chan")
    chan_index = lax.axis_index("chan")
    quarter = length // chan_count
    row_start = lax.axis_index(("rows", "sub")) * rows_block
    mask_float = residue_mask.astype(jnp.float32)
    own_mask = lax.dynamic_slice_in_dim(mask_float, row_start, rows_block)
    pair_mask = own_mask[None, :, None] * mask_float[None, None, :]

    def project(full_rows, layer_index):
        normed = (
            normalize(full_rows.astype(jnp.float32), 2) * in_gain[layer_index]
            + in_bias[layer_index]
        ).astype(jnp.bfloat16)
        projected = jnp.einsum(
            "ikc,qch->qhik", normed, projections[layer_index], preferred_element_type=jnp.float32
        )
        left_edges = (jax.nn.sigmoid(projected[0]) * projected[1] * pair_mask).astype(jnp.bfloat16)
        right_edges = (jax.nn.sigmoid(projected[2]) * projected[3] * pair_mask).astype(jnp.bfloat16)
        return (normed, left_edges, right_edges)

    def finish(triangle, normed, residual, layer_index):
        gathered = lax.all_to_all(triangle, "chan", split_axis=2, concat_axis=0, tiled=True)
        whole_float = gathered.astype(jnp.float32)
        scaled = (
            normalize(whole_float, 0) * out_gain[layer_index][:, None, None]
            + out_bias[layer_index][:, None, None]
        ).astype(jnp.bfloat16)
        update = jnp.einsum(
            "hij,hc->ijc", scaled, out_weight[layer_index], preferred_element_type=jnp.float32
        )
        normed_part = lax.dynamic_slice_in_dim(normed, chan_index * quarter, quarter, 1)
        gating = jax.nn.sigmoid(
            jnp.einsum(
                "ijc,cd->ijd",
                normed_part,
                gate_weight[layer_index],
                preferred_element_type=jnp.float32,
            )
        )
        return (residual.astype(jnp.float32) + gating * update).astype(jnp.bfloat16)

    normed, left_edges, right_edges = project(pair, 0)
    triangle = jnp.einsum(
        "hik,hjk->hij",
        left_edges,
        lax.all_gather(right_edges, ("rows", "sub"), axis=1, tiled=True),
        preferred_element_type=jnp.float32,
    ).astype(jnp.bfloat16)
    own_quarter = lax.dynamic_slice_in_dim(pair, chan_index * quarter, quarter, 1)
    layer_one = finish(triangle, normed, own_quarter, 0)
    full_rows = lax.all_gather(layer_one, "chan", axis=1, tiled=True)
    normed, left_edges, right_edges = project(full_rows, 1)
    left_cols, right_cols = (
        lax.all_to_all(left_edges, ("rows", "sub"), split_axis=2, concat_axis=1, tiled=True),
        lax.all_to_all(right_edges, ("rows", "sub"), split_axis=2, concat_axis=1, tiled=True),
    )
    triangle = jnp.einsum(
        "hki,hkj->hij",
        left_cols,
        lax.all_gather(right_cols, ("rows", "sub"), axis=2, tiled=True),
        preferred_element_type=jnp.float32,
    )
    return finish(triangle.astype(jnp.bfloat16), normed, layer_one, 1)


def swap(value, axis, step):
    count = lax.axis_size(axis)
    return lax.ppermute(value, axis, [(i, i ^ step) for i in range(count)])


def mm(a, b):
    return jnp.dot(a, b, preferred_element_type=jnp.float32)


def mmt(a, b):
    return lax.dot_general(a, b, (((1,), (1,)), ((), ())), preferred_element_type=jnp.float32)


def constants(c):
    average = jnp.full((c, c), 1.0 / c, jnp.float32)
    diagonal = lax.broadcasted_iota(jnp.int32, (c, c), 0) == lax.broadcasted_iota(jnp.int32, (c, c), 1)
    centring = jnp.where(diagonal, 1.0 - 1.0 / c, -1.0 / c)
    return centring.astype(jnp.bfloat16), average.astype(jnp.bfloat16)


def layer_norm(values, gain, bias, centring, average):
    centred = mm(values, centring)
    spread = mm((centred * centred).astype(jnp.bfloat16), average)
    return (centred * lax.rsqrt(spread + epsilon) * gain + bias).astype(jnp.bfloat16)


def gated(half_gate, half_value):
    return half_value * jnp.tanh(half_gate) + half_value


class Stage:
    def __init__(self, counts, state, small):
        self.left, self.right, self.turned, self.gate, self.z, self.tri, self.w, self.mask, self.gw, self.ow = state
        self.ig, self.ib = small
        self.rows_count, self.chan_count, self.sub_count, self.size = counts
        self.row = lax.axis_index("rows")
        self.chan = lax.axis_index("chan")
        self.sub = lax.axis_index("sub")
        self.length, _, self.c = self.z.shape
        self.h = self.left.shape[2]
        self.chip = self.size * self.sub_count
        self.centring, self.average = constants(self.c)

    def at(self, rs, ss):
        return ((self.row ^ rs) * self.sub_count + (self.sub ^ ss)) * self.size

    def tile(self, rs):
        return pl.multiple_of((self.row ^ rs) * self.chip, self.chip)

    def norm(self, x, layer):
        return layer_norm(x, self.ig[layer:layer + 1], self.ib[layer:layer + 1], self.centring, self.average)

    def edges(self, blocks):
        area = self.size * self.length
        x = jnp.concatenate([b.reshape(area, self.c) for _, b in blocks], 0)
        normed = self.norm(x, 0)
        places = [pl.ds(self.at(*where), self.size) for where, _ in blocks]
        both = [self.mask[p][:, None, :] * self.mask[...][None] for p in places]
        shape = (self.size, self.length, self.h)

        def part(v, i):
            return v[i * area:(i + 1) * area].reshape(shape)

        for ref, q in ((self.left, 0), (self.right, 2)):
            p = mmt(normed, self.w[0, q:q + 2].reshape(2 * self.h, self.c))
            for i, place in enumerate(places):
                ref[place] = gated(part(p[:, :self.h], i), part(p[:, self.h:], i) * both[i])
        g = jnp.tanh(mm(normed, self.gw[0]))
        for i, place in enumerate(places):
            self.gate[place] = part(g, i)
            self.z[place] = part(x.astype(jnp.float32), i)

    def turn(self, rs):
        tile = self.tile(rs)
        self.turned[:, pl.ds(tile, self.chip), :] = jnp.swapaxes(self.right[pl.ds(tile, self.chip)], 0, 1)

    def triangle(self, ks, chips):
        tiles = [pl.ds(self.tile(rs), self.chip) for rs in chips]

        def inner(m, acc):
            rs = [self.turned[m, t, :] for t in tiles]
            out = []
            for i, k in enumerate(ks):
                l = self.left[k, pl.ds(m, 1), :]
                out += [acc[i * len(rs) + j] + l * r for j, r in enumerate(rs)]
            return tuple(out)

        zero = tuple(jnp.zeros((self.chip, self.h), jnp.float32) for _ in range(len(ks) * len(tiles)))
        acc = lax.fori_loop(0, self.length, inner, zero, unroll=8)
        for i, k in enumerate(ks):
            for j, t in enumerate(tiles):
                self.tri[k, t, :] = acc[i * len(tiles) + j]

    def block_rows(self, *places):
        return [self.at(*p) + i for p in places for i in range(self.size)]

    def chip_rows(self, rs):
        return [self.tile(rs) + i for i in range(self.chip)]


def first_kernel(counts, where, *refs):
    chan_count = counts[1]
    n = len(where)
    blocks, weights = refs[:n], refs[n:n + chan_count]
    mask_ref, ig_ref, ib_ref, pair_hbm, gw_hbm, ow_hbm = refs[n + chan_count:n + chan_count + 6]
    state = refs[n + chan_count + 6:n + chan_count + 16]
    pair_ref, gw_raw, ow_raw, sems = refs[n + chan_count + 16:]
    pairs = ((pair_hbm, pair_ref), (gw_hbm, gw_raw), (ow_hbm, ow_raw))
    copies = [pltpu.make_async_copy(src, dst, sems.at[i]) for i, (src, dst) in enumerate(pairs)]
    for copy in copies:
        copy.start()
    s = Stage(counts, state, (ig_ref, ib_ref))
    part = s.h // chan_count
    half = jnp.bfloat16(0.5)
    for i in range(chan_count):
        at = pl.multiple_of((s.chan ^ i) * part, part)
        s.w[:, :, pl.ds(at, part), :] = weights[i][...] * half
    across = mask_ref[...].astype(jnp.float32)
    square = (s.length, s.length)
    diagonal = lax.broadcasted_iota(jnp.int32, square, 0) == lax.broadcasted_iota(jnp.int32, square, 1)
    s.mask[...] = mm(jnp.where(diagonal, across, 0.0).astype(jnp.bfloat16), jnp.ones((s.length, s.h), jnp.bfloat16))
    copies[1].wait()
    s.gw[...] = gw_raw[...] * half
    copies[0].wait()
    s.edges([((0, 0), pair_ref[...])] + [(w, b[...]) for w, b in zip(where, blocks)])
    copies[2].wait()
    s.ow[...] = ow_raw[...] * half
    for rs in (0, 1):
        s.turn(rs)
    for rs in (0, 1):
        s.triangle(s.chip_rows(rs), (0, 1))


def next_kernel(counts, where, block_ref, ig_ref, ib_ref, *refs):
    s = Stage(counts, refs[len(refs) // 2:], (ig_ref, ib_ref))
    size = counts[3]
    s.edges([(w, block_ref[i * size:(i + 1) * size]) for i, w in enumerate(where)])
    s.triangle(s.block_rows(*where), (0, 1))


def last_kernel(counts, where, block_ref, ig_ref, ib_ref, *refs):
    state = refs[:10]
    og_hbm, ob_hbm, out_ref, l1_ref, r1_ref, n1_ref, og_ref, ob_ref, sems = refs[10:]
    copies = [pltpu.make_async_copy(og_hbm, og_ref, sems.at[0]), pltpu.make_async_copy(ob_hbm, ob_ref, sems.at[1])]
    for copy in copies:
        copy.start()
    s = Stage(counts, state, (ig_ref, ib_ref))
    size, length, c, h = s.size, s.length, s.c, s.h
    quarter = length // s.chan_count
    s.edges([(w, block_ref[i * size:(i + 1) * size]) for i, w in enumerate(where)])
    s.triangle(s.block_rows(*where), (0, 1))
    others = tuple(range(2, s.rows_count))
    for rs in others:
        s.turn(rs)
    for rs in range(s.rows_count):
        s.triangle(s.chip_rows(rs), others)

    def finish(tri, half_gate, residual, layer):
        scaled = layer_norm(
            tri.astype(jnp.bfloat16), og_ref[layer:layer + 1], ob_ref[layer:layer + 1], s.centring, s.average
        )
        update = mm(scaled, s.ow[layer])
        return residual + (update * half_gate + update)

    for copy in copies:
        copy.wait()
    chunk = length // 2
    for b in range(2):
        rows = slice(b * chunk, (b + 1) * chunk)
        flat = (chunk * length, c)
        z = finish(s.tri[rows].reshape(flat), s.gate[rows].reshape(flat), s.z[rows].reshape(flat), 0)
        s.z[rows] = z.astype(jnp.bfloat16).astype(jnp.float32).reshape(chunk, length, c)

    own = s.at(0, 0)
    i_tile = s.tile(0)
    j_at = pl.multiple_of(s.chan * quarter, quarter)
    mask = s.mask[...]
    zi = s.z[:, pl.ds(i_tile, s.chip), :].reshape(length * s.chip, c).astype(jnp.bfloat16)
    mi = mask[:, None, :] * s.mask[pl.ds(i_tile, s.chip)][None]
    p = mmt(s.norm(zi, 1), s.w[1, 0:2].reshape(2 * h, c))
    shape = (length, s.chip, h)
    l1_ref[...] = gated(p[:, :h].reshape(shape), p[:, h:].reshape(shape) * mi)
    zj = s.z[:, pl.ds(j_at, quarter), :].reshape(length * quarter, c).astype(jnp.bfloat16)
    nj = s.norm(zj, 1)
    mj = mask[:, None, :] * s.mask[pl.ds(j_at, quarter)][None]
    p = mmt(nj, s.w[1, 2:4].reshape(2 * h, c))
    shape = (length, quarter, h)
    r1_ref[...] = gated(p[:, :h].reshape(shape), p[:, h:].reshape(shape) * mj)
    n1_ref[...] = nj.reshape(shape)

    first = own - i_tile

    def inner(k, acc):
        r = r1_ref[k]
        return tuple(a + l1_ref[k, pl.ds(first + i, 1), :] * r for i, a in enumerate(acc))

    zero = tuple(jnp.zeros((quarter, h), jnp.float32) for _ in range(size))
    tri = jnp.concatenate(lax.fori_loop(0, length, inner, zero, unroll=8), 0)
    mine = pl.ds(own, size)
    flat = (size * quarter, c)
    gate = jnp.tanh(mm(n1_ref[mine].reshape(flat), s.gw[1]))
    z = finish(tri, gate, s.z[mine, pl.ds(j_at, quarter), :].reshape(flat), 1)
    out_ref[...] = z.astype(jnp.bfloat16).reshape(size, quarter, c)


def in_vmem(value):
    return pltpu.with_memory_space_constraint(value, pltpu.VMEM)


def in_hbm(value):
    return pltpu.with_memory_space_constraint(value, pltpu.HBM)


VMEM = pl.BlockSpec(memory_space=pltpu.VMEM)
HBM = pl.BlockSpec(memory_space=pltpu.HBM)


def join_kernel(a_ref, b_ref, out_ref):
    size = a_ref.shape[0]
    out_ref[0:size] = a_ref[...]
    out_ref[size:] = b_ref[...]


def join(a, b):
    return pl.pallas_call(
        join_kernel,
        out_shape=pltpu.VMEM((2 * a.shape[0], *a.shape[1:]), a.dtype),
        in_specs=[VMEM, VMEM],
        out_specs=VMEM,
        compiler_params=pltpu.CompilerParams(vmem_limit_bytes=1 << 20),
    )(in_vmem(a), in_vmem(b))


def gathered(
    pair, residue_mask, in_gain, in_bias, projections, gate_weight, out_gain, out_bias, out_weight
):
    rows_count, chan_count, sub_count = (lax.axis_size(a) for a in ("rows", "chan", "sub"))
    size, length, c = pair.shape
    h = out_weight.shape[1]
    counts = (rows_count, chan_count, sub_count, size)
    turned = jnp.swapaxes(projections, 2, 3)
    cross = [
        (r * sub_count + s, (r ^ 1) * sub_count + (s ^ 1)) for r in range(rows_count) for s in range(sub_count)
    ]
    first = lax.ppermute(pair, ("rows", "sub"), cross)
    beside = swap(pair, "sub", 1)
    weights = [turned] + [swap(turned, "chan", i) for i in range(1, chan_count)]
    joined = join(beside, first)
    away = swap(joined, "rows", 2)
    back = swap(first, "sub", 1)
    last = swap(away, "sub", 1)

    wide = (length, length, c)
    state = [
        jax.ShapeDtypeStruct(shape, dtype)
        for shape, dtype in (
            *[(wide, jnp.float32)] * 6,
            ((2, 4, h, c), jnp.bfloat16),
            ((length, h), jnp.float32),
            ((2, c, c), jnp.bfloat16),
            ((2, h, c), jnp.bfloat16),
        )
    ]
    held = [pltpu.VMEM(t.shape, t.dtype) for t in state]
    small = [in_gain, in_bias]

    def params(mib):
        return pltpu.CompilerParams(vmem_limit_bytes=mib << 20)

    def cost(rows):
        return pl.CostEstimate(flops=rows * 128 * 128 * 16, bytes_accessed=0, transcendentals=0)

    near = [beside, first, back, *weights, residue_mask[None], *small]
    far = [pair, gate_weight, out_weight]
    state = pl.pallas_call(
        functools.partial(first_kernel, counts, ((0, 1), (1, 1), (1, 0))),
        out_shape=held,
        in_specs=[VMEM] * len(near) + [HBM] * len(far),
        out_specs=[VMEM] * len(held),
        scratch_shapes=[
            *[pltpu.VMEM(o.shape, o.dtype) for o in far],
            pltpu.SemaphoreType.DMA((len(far),)),
        ],
        compiler_params=params(8),
        cost_estimate=cost(512 * 64),
    )(*[in_vmem(o) for o in near], *[in_hbm(o) for o in far])
    near = [away, *small]
    state = pl.pallas_call(
        functools.partial(next_kernel, counts, ((2, 1), (3, 1))),
        out_shape=held,
        in_specs=[VMEM] * (len(near) + len(held)),
        out_specs=[VMEM] * len(held),
        input_output_aliases={len(near) + i: i for i in range(len(held))},
        compiler_params=params(8),
        cost_estimate=cost(256 * 64),
    )(*[in_vmem(o) for o in near], *[in_vmem(o) for o in state])
    near = [last, *small]
    far = [out_gain, out_bias]
    return pl.pallas_call(
        functools.partial(last_kernel, counts, ((2, 0), (3, 0))),
        out_shape=jax.ShapeDtypeStruct((size, length // chan_count, c), jnp.bfloat16),
        in_specs=[VMEM] * (len(near) + len(held)) + [HBM] * len(far),
        out_specs=VMEM,
        scratch_shapes=[
            pltpu.VMEM((length, size * sub_count, h), jnp.float32),
            pltpu.VMEM((length, length // chan_count, h), jnp.float32),
            pltpu.VMEM((length, length // chan_count, h), jnp.bfloat16),
            *[pltpu.VMEM(o.shape, o.dtype) for o in far],
            pltpu.SemaphoreType.DMA((len(far),)),
        ],
        compiler_params=params(16),
        cost_estimate=cost(1024),
    )(*[in_vmem(o) for o in near], *[in_vmem(o) for o in state], *[in_hbm(o) for o in far])


def solution(mesh):
    def body(pair, *rest):
        size, length, c = pair.shape
        small = 2 * length * length * c <= GATHER_LIMIT
        fits = mesh.shape["sub"] == 2 and mesh.shape["rows"] == 4 and size * 2 == 8
        chans = mesh.shape["chan"]
        if not (small and fits and chans & (chans - 1) == 0):
            return shards(pair, *rest)
        return gathered(pair, *rest)

    placed = (
        P(("crops", "rows", "sub"), None, None),
        P("crops"),
        P(),
        P(),
        P(None, None, None, "chan"),
        P(),
        P(),
        P(),
        P(),
    )
    return jax.shard_map(
        body,
        mesh=mesh,
        in_specs=placed,
        out_specs=P(("crops", "rows", "sub"), "chan", None),
        check_vma=False,
    )
```

```python
import functools

import jax
import jax.numpy as jnp
from jax import lax
from jax.experimental import pallas as pl
from jax.experimental.pallas import tpu as pltpu
from jax.sharding import PartitionSpec as P


epsilon = 1e-05


GATHER_LIMIT = 1 << 20


def normalize(values, reduce_axis):
    centre = jnp.mean(values, axis=reduce_axis, keepdims=True)
    centred = values - centre
    spread = jnp.mean(centred * centred, axis=reduce_axis, keepdims=True)
    return centred * lax.rsqrt(spread + epsilon)


def shards(
    pair, residue_mask, in_gain, in_bias, projections, gate_weight, out_gain, out_bias, out_weight
):
    rows_block = pair.shape[0]
    length = pair.shape[1]
    chan_count = lax.axis_size("chan")
    chan_index = lax.axis_index("chan")
    quarter = length // chan_count
    row_start = lax.axis_index(("rows", "sub")) * rows_block
    mask_float = residue_mask.astype(jnp.float32)
    own_mask = lax.dynamic_slice_in_dim(mask_float, row_start, rows_block)
    pair_mask = own_mask[None, :, None] * mask_float[None, None, :]

    def project(full_rows, layer_index):
        normed = (
            normalize(full_rows.astype(jnp.float32), 2) * in_gain[layer_index]
            + in_bias[layer_index]
        ).astype(jnp.bfloat16)
        projected = jnp.einsum(
            "ikc,qch->qhik", normed, projections[layer_index], preferred_element_type=jnp.float32
        )
        left_edges = (jax.nn.sigmoid(projected[0]) * projected[1] * pair_mask).astype(jnp.bfloat16)
        right_edges = (jax.nn.sigmoid(projected[2]) * projected[3] * pair_mask).astype(jnp.bfloat16)
        return (normed, left_edges, right_edges)

    def finish(triangle, normed, residual, layer_index):
        gathered = lax.all_to_all(triangle, "chan", split_axis=2, concat_axis=0, tiled=True)
        whole_float = gathered.astype(jnp.float32)
        scaled = (
            normalize(whole_float, 0) * out_gain[layer_index][:, None, None]
            + out_bias[layer_index][:, None, None]
        ).astype(jnp.bfloat16)
        update = jnp.einsum(
            "hij,hc->ijc", scaled, out_weight[layer_index], preferred_element_type=jnp.float32
        )
        normed_part = lax.dynamic_slice_in_dim(normed, chan_index * quarter, quarter, 1)
        gating = jax.nn.sigmoid(
            jnp.einsum(
                "ijc,cd->ijd",
                normed_part,
                gate_weight[layer_index],
                preferred_element_type=jnp.float32,
            )
        )
        return (residual.astype(jnp.float32) + gating * update).astype(jnp.bfloat16)

    normed, left_edges, right_edges = project(pair, 0)
    triangle = jnp.einsum(
        "hik,hjk->hij",
        left_edges,
        lax.all_gather(right_edges, ("rows", "sub"), axis=1, tiled=True),
        preferred_element_type=jnp.float32,
    ).astype(jnp.bfloat16)
    own_quarter = lax.dynamic_slice_in_dim(pair, chan_index * quarter, quarter, 1)
    layer_one = finish(triangle, normed, own_quarter, 0)
    full_rows = lax.all_gather(layer_one, "chan", axis=1, tiled=True)
    normed, left_edges, right_edges = project(full_rows, 1)
    left_cols, right_cols = (
        lax.all_to_all(left_edges, ("rows", "sub"), split_axis=2, concat_axis=1, tiled=True),
        lax.all_to_all(right_edges, ("rows", "sub"), split_axis=2, concat_axis=1, tiled=True),
    )
    triangle = jnp.einsum(
        "hki,hkj->hij",
        left_cols,
        lax.all_gather(right_cols, ("rows", "sub"), axis=2, tiled=True),
        preferred_element_type=jnp.float32,
    )
    return finish(triangle.astype(jnp.bfloat16), normed, layer_one, 1)


def swap(value, axis, step):
    count = lax.axis_size(axis)
    return lax.ppermute(value, axis, [(i, i ^ step) for i in range(count)])


def mm(a, b):
    return jnp.dot(a, b, preferred_element_type=jnp.float32)


def mmt(a, b):
    return lax.dot_general(a, b, (((1,), (1,)), ((), ())), preferred_element_type=jnp.float32)


def constants(c):
    average = jnp.full((c, c), 1.0 / c, jnp.float32)
    diagonal = lax.broadcasted_iota(jnp.int32, (c, c), 0) == lax.broadcasted_iota(jnp.int32, (c, c), 1)
    centring = jnp.where(diagonal, 1.0 - 1.0 / c, -1.0 / c)
    return centring.astype(jnp.bfloat16), average.astype(jnp.bfloat16)


def layer_norm(values, gain, bias, centring, average):
    centred = mm(values, centring)
    spread = mm((centred * centred).astype(jnp.bfloat16), average)
    return (centred * lax.rsqrt(spread + epsilon) * gain + bias).astype(jnp.bfloat16)


def gated(half_gate, half_value):
    return half_value * jnp.tanh(half_gate) + half_value


class Stage:
    def __init__(self, counts, state, small):
        (self.left, self.right, self.turned, self.gate, self.x, self.tri, self.w, self.mask, self.gw, self.ow) = state
        self.ig, self.ib = small
        self.rows_count, self.chan_count, self.sub_count, self.size = counts
        self.row = lax.axis_index("rows")
        self.chan = lax.axis_index("chan")
        self.sub = lax.axis_index("sub")
        self.length, _, self.c = self.x.shape
        self.h = self.mask.shape[1]
        self.chip = self.size * self.sub_count
        self.quarter = self.length // self.chan_count
        self.centring, self.average = constants(self.c)

    def at(self, rs, ss):
        return ((self.row ^ rs) * self.sub_count + (self.sub ^ ss)) * self.size

    def halves(self, ss):
        return [
            self.chan * self.quarter + i * self.chip + (self.sub ^ ss) * self.size
            for i in range(self.quarter // self.chip)
        ]

    def slots(self):
        return [[self.at(0, 0) - self.sub * self.size + i * self.size for i in range(self.sub_count)],
                self.halves(0), self.halves(1)]

    def norm(self, x, layer):
        return layer_norm(x, self.ig[layer:layer + 1], self.ib[layer:layer + 1], self.centring, self.average)

    def keep(self, step, ref):
        part = self.h // self.chan_count
        at = pl.multiple_of((self.chan ^ step) * part, part)
        self.w[:, :, pl.ds(at, part), :] = ref[...] * jnp.bfloat16(0.5)

    def places(self, where):
        return [pl.ds(self.at(*w), self.size) for w in where]

    def part(self, value, i):
        area = self.size * self.length
        return value[i * area:(i + 1) * area].reshape(self.size, self.length, value.shape[1])

    def enter(self, where, blocks):
        area = self.size * self.length
        x = jnp.concatenate([b.reshape(area, self.c) for b in blocks], 0)
        normed = self.norm(x, 0)
        g = jnp.tanh(mm(normed, self.gw[0]))
        for i, place in enumerate(self.places(where)):
            self.gate[place] = self.part(g, i)
            self.x[place] = self.part(x.astype(jnp.float32), i)
        return normed

    def edges(self, where, normed):
        places = self.places(where)
        both = [self.mask[p][:, None, :] * self.mask[...][None] for p in places]
        for ref, q in ((self.left, 0), (self.right, 2)):
            p = mmt(normed, self.w[0, q:q + 2].reshape(2 * self.h, self.c))
            for i, place in enumerate(places):
                ref[place] = gated(self.part(p[:, :self.h], i), self.part(p[:, self.h:], i) * both[i])

    def turn(self, slot):
        rows = jnp.concatenate([self.right[pl.ds(o, self.size)] for o in self.slots()[slot]], 0)
        self.turned[slot] = jnp.swapaxes(rows, 0, 1)

    def triangle(self, ks, slots):
        def inner(m, acc):
            rs = [self.turned[t, m] for t in slots]
            out = []
            for i, k in enumerate(ks):
                l = self.left[k, pl.ds(m, 1), :]
                out += [acc[i * len(rs) + j] + l * r for j, r in enumerate(rs)]
            return tuple(out)

        zero = tuple(jnp.zeros((self.chip, self.h), jnp.float32) for _ in range(len(ks) * len(slots)))
        acc = lax.fori_loop(0, self.length, inner, zero, unroll=8)
        for i, k in enumerate(ks):
            for j, t in enumerate(slots):
                self.tri[t, k] = acc[i * len(slots) + j]

    def block_rows(self, places):
        return [self.at(*p) + i for p in places for i in range(self.size)]

    def columns(self, ref, slot):
        return jnp.concatenate([ref[:, pl.ds(o, self.size), :] for o in self.slots()[slot]], 1)

    def mask_rows(self, slot):
        return jnp.concatenate([self.mask[pl.ds(o, self.size)] for o in self.slots()[slot]], 0)


def early_kernel(counts, *refs):
    mask_ref, ig_ref, ib_ref, pair_hbm, w_hbm, gw_hbm, ow_hbm = refs[:7]
    gate, x, w, mask, gw, ow, normed = refs[7:14]
    raw, sems = refs[14:18], refs[18]
    copies = [pltpu.make_async_copy(a, b, sems.at[i]) for i, (a, b) in enumerate(zip((pair_hbm, w_hbm, gw_hbm, ow_hbm), raw))]
    for copy in copies:
        copy.start()
    s = Stage(counts, (mask, None, None, gate, x, None, w, mask, gw, ow), (ig_ref, ib_ref))
    half = jnp.bfloat16(0.5)
    across = mask_ref[...].astype(jnp.float32)
    square = (s.length, s.length)
    diagonal = lax.broadcasted_iota(jnp.int32, square, 0) == lax.broadcasted_iota(jnp.int32, square, 1)
    mask[...] = mm(jnp.where(diagonal, across, 0.0).astype(jnp.bfloat16), jnp.ones((s.length, s.h), jnp.bfloat16))
    for copy in copies:
        copy.wait()
    pair_ref, w_ref, gw_ref, ow_ref = raw
    gw[...] = gw_ref[...] * half
    ow[...] = ow_ref[...] * half
    s.keep(0, w_ref)
    normed[...] = s.enter(((0, 0),), (pair_ref[...],))


def first_kernel(counts, where, *refs):
    n = len(where) - 1
    others = counts[1] - 1
    blocks, weights = refs[:n], refs[n:n + others]
    ig_ref, ib_ref, normed_ref, mask_in, gw_in = refs[n + others:n + others + 5]
    left, right, turned, tri, gate, x, w = refs[n + others + 8:]
    s = Stage(counts, (left, right, turned, gate, x, tri, w, mask_in, gw_in, None), (ig_ref, ib_ref))
    for i, ref in enumerate(weights):
        s.keep(i + 1, ref)
    normed = s.enter(where[1:], [b[...] for b in blocks])
    s.edges(where, jnp.concatenate([normed_ref[...], normed], 0))
    s.turn(0)
    s.turn(1)
    ks = s.block_rows(where)
    middle = len(ks) // 2
    s.triangle(ks[:middle], (0, 1))
    s.triangle(ks[middle:], (0, 1))


def last_kernel(counts, where, *refs):
    n = len(where)
    blocks = refs[:n]
    ig_ref, ib_ref = refs[n:n + 2]
    state = refs[n + 2:n + 12]
    og_hbm, ob_hbm, out_ref, z_ref, l1_ref, r1_ref, og_ref, ob_ref, sems = refs[n + 12:]
    copies = [pltpu.make_async_copy(og_hbm, og_ref, sems.at[0]), pltpu.make_async_copy(ob_hbm, ob_ref, sems.at[1])]
    for copy in copies:
        copy.start()
    s = Stage(counts, state, (ig_ref, ib_ref))
    size, length, c, h, chip, quarter = s.size, s.length, s.c, s.h, s.chip, s.quarter
    s.edges(where, s.enter(where, [b[...] for b in blocks]))
    s.turn(2)
    s.triangle(s.block_rows(where), (0, 1))
    middle = length // 2
    s.triangle(range(middle), (2,))
    s.triangle(range(middle, length), (2,))
    for copy in copies:
        copy.wait()

    def finish(tri, half_gate, residual, layer):
        scaled = layer_norm(
            tri.astype(jnp.bfloat16), og_ref[layer:layer + 1], ob_ref[layer:layer + 1], s.centring, s.average
        )
        update = mm(scaled, s.ow[layer])
        return (residual + (update * half_gate + update)).astype(jnp.bfloat16)

    area = length * chip
    half_gate = jnp.concatenate([s.columns(s.gate, t).reshape(area, c) for t in range(3)], 0)
    residual = jnp.concatenate([s.columns(s.x, t).reshape(area, c) for t in range(3)], 0)
    z = finish(s.tri[...].reshape(3 * area, h), half_gate, residual, 0)
    z_ref[...] = z.astype(jnp.float32).reshape(3, length, chip, c)

    mask = s.mask[...][:, None, :]
    normed = s.norm(z, 1)
    shape = (length, chip, h)
    p = mmt(normed[:area], s.w[1, 0:2].reshape(2 * h, c))
    l1_ref[...] = gated(p[:, :h].reshape(shape), p[:, h:].reshape(shape) * (mask * s.mask_rows(0)[None]))
    p = mmt(normed[area:], s.w[1, 2:4].reshape(2 * h, c))
    for t in (1, 2):
        at = slice((t - 1) * area, t * area)
        r1_ref[t - 1] = gated(p[at, :h].reshape(shape), p[at, h:].reshape(shape) * (mask * s.mask_rows(t)[None]))
    own = s.at(0, 0)
    mine = z_ref[1:3, pl.ds(own, size)].reshape(2 * size * chip, c)
    half_gate = jnp.tanh(mm(s.norm(mine.astype(jnp.bfloat16), 1), s.gw[1]))

    first = s.sub * size

    def inner(k, acc):
        rs = [r1_ref[t, k] for t in range(2)]
        ls = [l1_ref[k, pl.ds(first + i, 1), :] for i in range(size)]
        return tuple(acc[t * size + i] + ls[i] * rs[t] for t in range(2) for i in range(size))

    zero = tuple(jnp.zeros((chip, h), jnp.float32) for _ in range(2 * size))
    tri = jnp.concatenate(lax.fori_loop(0, length, inner, zero, unroll=8), 0)
    z = finish(tri, half_gate, mine, 1).astype(jnp.float32).reshape(2, size, chip, c)
    even = jnp.where(s.sub == 0, z[0], z[1])
    odd = jnp.where(s.sub == 0, z[1], z[0])
    rows = [v[:, i * size:(i + 1) * size] for i in range(quarter // chip) for v in (even, odd)]
    out_ref[...] = jnp.concatenate(rows, 1).astype(jnp.bfloat16)


def in_vmem(value):
    return pltpu.with_memory_space_constraint(value, pltpu.VMEM)


def in_hbm(value):
    return pltpu.with_memory_space_constraint(value, pltpu.HBM)


VMEM = pl.BlockSpec(memory_space=pltpu.VMEM)
HBM = pl.BlockSpec(memory_space=pltpu.HBM)


def gathered(
    pair, residue_mask, in_gain, in_bias, projections, gate_weight, out_gain, out_bias, out_weight
):
    rows_count, chan_count, sub_count = (lax.axis_size(a) for a in ("rows", "chan", "sub"))
    size, length, c = pair.shape
    h = out_weight.shape[1]
    counts = (rows_count, chan_count, sub_count, size)
    turned = jnp.swapaxes(projections, 2, 3)
    hops = tuple(range(1, rows_count))
    far, near = {}, {}
    for rs in hops:
        far[rs] = swap(pair, "rows", rs)
    near[0] = swap(pair, "sub", 1)
    weights = [swap(turned, "chan", i) for i in range(1, chan_count)]
    for rs in hops:
        near[rs] = swap(far[rs], "sub", 1)

    wide = pltpu.VMEM((length, length, c), jnp.float32)
    tiles = pltpu.VMEM((3, length, size * sub_count, h), jnp.float32)
    small = [residue_mask[None], in_gain, in_bias]

    def call(kernel, near, far, out_shape, scratch=(), aliases={}, rows=0, mib=8):
        return pl.pallas_call(
            kernel,
            out_shape=out_shape,
            in_specs=[VMEM] * len(near) + [HBM] * len(far),
            out_specs=jax.tree.map(lambda _: VMEM, out_shape),
            scratch_shapes=[
                *scratch,
                *[pltpu.VMEM(o.shape, o.dtype) for o in far],
                *([pltpu.SemaphoreType.DMA((len(far),))] if far else []),
            ],
            input_output_aliases=aliases,
            compiler_params=pltpu.CompilerParams(vmem_limit_bytes=mib << 20),
            cost_estimate=pl.CostEstimate(flops=rows * c * c * 16, bytes_accessed=0, transcendentals=0),
        )(*[in_vmem(o) for o in near], *[in_hbm(o) for o in far])

    gate, x, w, mask, gw, ow, normed = call(
        functools.partial(early_kernel, counts),
        small,
        [pair, turned, gate_weight, out_weight],
        [
            wide,
            wide,
            pltpu.VMEM((2, 4, h, c), jnp.bfloat16),
            pltpu.VMEM((length, h), jnp.float32),
            pltpu.VMEM((2, c, c), jnp.bfloat16),
            pltpu.VMEM((2, h, c), jnp.bfloat16),
            pltpu.VMEM((size * length, c), jnp.bfloat16),
        ],
        rows=length * length,
    )
    where = ((0, 0), (0, 1), *[(rs, 0) for rs in hops])
    near_one = [near[0], *[far[rs] for rs in hops], *weights, in_gain, in_bias, normed, mask, gw, gate, x, w]
    left, right, folded, tri, gate, x, w = call(
        functools.partial(first_kernel, counts, where),
        near_one,
        [],
        [wide, wide, tiles, tiles, wide, wide, pltpu.VMEM(w.shape, w.dtype)],
        aliases={len(near_one) - 3 + i: 4 + i for i in range(3)},
        rows=length * length,
    )
    state = [left, right, folded, gate, x, tri, w, mask, gw, ow]
    return call(
        functools.partial(last_kernel, counts, tuple((rs, 1) for rs in hops)),
        [*[near[rs] for rs in hops], in_gain, in_bias, *state],
        [out_gain, out_bias],
        jax.ShapeDtypeStruct((size, length // chan_count, c), jnp.bfloat16),
        scratch=[
            pltpu.VMEM((3, length, size * sub_count, c), jnp.float32),
            pltpu.VMEM((length, size * sub_count, h), jnp.float32),
            pltpu.VMEM((2, length, size * sub_count, h), jnp.float32),
        ],
        rows=1,
        mib=16,
    )


def solution(mesh):
    def body(pair, *rest):
        size, length, c = pair.shape
        small = 2 * length * length * c <= GATHER_LIMIT
        fits = (
            mesh.shape["sub"] == 2
            and mesh.shape["rows"] & (mesh.shape["rows"] - 1) == 0
            and size * 2 == 8
            and length == 16 * mesh.shape["chan"]
        )
        if not (small and fits):
            return shards(pair, *rest)
        return gathered(pair, *rest)

    placed = (
        P(("crops", "rows", "sub"), None, None),
        P("crops"),
        P(),
        P(),
        P(None, None, None, "chan"),
        P(),
        P(),
        P(),
        P(),
    )
    step = jax.shard_map(
        body,
        mesh=mesh,
        in_specs=placed,
        out_specs=P(("crops", "rows", "sub"), "chan", None),
        check_vma=False,
    )
    if 8 * mesh.shape["rows"] != 16 * mesh.shape["chan"]:
        return step
    return step
```

```python
import functools

import jax
import jax.numpy as jnp
from jax import lax
from jax.experimental import pallas as pl
from jax.experimental.pallas import tpu as pltpu
from jax.sharding import PartitionSpec as P


epsilon = 1e-05


GATHER_LIMIT = 1 << 20


def normalize(values, reduce_axis):
    centre = jnp.mean(values, axis=reduce_axis, keepdims=True)
    centred = values - centre
    spread = jnp.mean(centred * centred, axis=reduce_axis, keepdims=True)
    return centred * lax.rsqrt(spread + epsilon)


def shards(
    pair, residue_mask, in_gain, in_bias, projections, gate_weight, out_gain, out_bias, out_weight
):
    rows_block = pair.shape[0]
    length = pair.shape[1]
    chan_count = lax.axis_size("chan")
    chan_index = lax.axis_index("chan")
    quarter = length // chan_count
    row_start = lax.axis_index(("rows", "sub")) * rows_block
    mask_float = residue_mask.astype(jnp.float32)
    own_mask = lax.dynamic_slice_in_dim(mask_float, row_start, rows_block)
    pair_mask = own_mask[None, :, None] * mask_float[None, None, :]

    def project(full_rows, layer_index):
        normed = (
            normalize(full_rows.astype(jnp.float32), 2) * in_gain[layer_index]
            + in_bias[layer_index]
        ).astype(jnp.bfloat16)
        projected = jnp.einsum(
            "ikc,qch->qhik", normed, projections[layer_index], preferred_element_type=jnp.float32
        )
        left_edges = (jax.nn.sigmoid(projected[0]) * projected[1] * pair_mask).astype(jnp.bfloat16)
        right_edges = (jax.nn.sigmoid(projected[2]) * projected[3] * pair_mask).astype(jnp.bfloat16)
        return (normed, left_edges, right_edges)

    def finish(triangle, normed, residual, layer_index):
        gathered = lax.all_to_all(triangle, "chan", split_axis=2, concat_axis=0, tiled=True)
        whole_float = gathered.astype(jnp.float32)
        scaled = (
            normalize(whole_float, 0) * out_gain[layer_index][:, None, None]
            + out_bias[layer_index][:, None, None]
        ).astype(jnp.bfloat16)
        update = jnp.einsum(
            "hij,hc->ijc", scaled, out_weight[layer_index], preferred_element_type=jnp.float32
        )
        normed_part = lax.dynamic_slice_in_dim(normed, chan_index * quarter, quarter, 1)
        gating = jax.nn.sigmoid(
            jnp.einsum(
                "ijc,cd->ijd",
                normed_part,
                gate_weight[layer_index],
                preferred_element_type=jnp.float32,
            )
        )
        return (residual.astype(jnp.float32) + gating * update).astype(jnp.bfloat16)

    normed, left_edges, right_edges = project(pair, 0)
    triangle = jnp.einsum(
        "hik,hjk->hij",
        left_edges,
        lax.all_gather(right_edges, ("rows", "sub"), axis=1, tiled=True),
        preferred_element_type=jnp.float32,
    ).astype(jnp.bfloat16)
    own_quarter = lax.dynamic_slice_in_dim(pair, chan_index * quarter, quarter, 1)
    layer_one = finish(triangle, normed, own_quarter, 0)
    full_rows = lax.all_gather(layer_one, "chan", axis=1, tiled=True)
    normed, left_edges, right_edges = project(full_rows, 1)
    left_cols, right_cols = (
        lax.all_to_all(left_edges, ("rows", "sub"), split_axis=2, concat_axis=1, tiled=True),
        lax.all_to_all(right_edges, ("rows", "sub"), split_axis=2, concat_axis=1, tiled=True),
    )
    triangle = jnp.einsum(
        "hki,hkj->hij",
        left_cols,
        lax.all_gather(right_cols, ("rows", "sub"), axis=2, tiled=True),
        preferred_element_type=jnp.float32,
    )
    return finish(triangle.astype(jnp.bfloat16), normed, layer_one, 1)


def swap(value, axis, step):
    count = lax.axis_size(axis)
    return lax.ppermute(value, axis, [(i, i ^ step) for i in range(count)])


def mm(a, b):
    return jnp.dot(a, b, preferred_element_type=jnp.float32)


def mmt(a, b):
    return lax.dot_general(a, b, (((1,), (1,)), ((), ())), preferred_element_type=jnp.float32)


def constants(c):
    diagonal = lax.broadcasted_iota(jnp.int32, (c, c), 0) == lax.broadcasted_iota(jnp.int32, (c, c), 1)
    return jnp.where(diagonal, 1.0 - 1.0 / c, -1.0 / c).astype(jnp.bfloat16)


def exact(a, b):
    total = 0.0
    for _ in range(3):
        piece = a.astype(jnp.bfloat16)
        total = total + mm(piece, b)
        a = a - piece.astype(jnp.float32)
    return total


def layer_norm(values, gain, bias, centring):
    centred = mm(values, centring)
    spread = jnp.mean(centred * centred, axis=1, keepdims=True)
    return (centred * lax.rsqrt(spread + epsilon) * gain + bias).astype(jnp.bfloat16)


def gated(half_gate, half_value):
    return half_value * jnp.tanh(half_gate) + half_value


class Place:
    def __init__(self, counts, length, c):
        self.rows_count, self.chan_count, self.sub_count, self.size = counts
        self.length, self.c = length, c
        self.row = lax.axis_index("rows")
        self.chan = lax.axis_index("chan")
        self.sub = lax.axis_index("sub")
        self.chip = self.size * self.sub_count
        self.quarter = length // self.chan_count
        self.area = self.size * length
        self.centring = constants(c)
        hops = range(1, self.rows_count)
        self.early = [(0, 0), *[(rs, 0) for rs in hops], (0, 1)]
        self.late = [(rs, 1) for rs in hops]

    def at(self, rs, ss):
        return ((self.row ^ rs) * self.sub_count + (self.sub ^ ss)) * self.size

    def chips(self):
        return [(self.chan * (self.quarter // self.chip) + i) ^ self.row for i in range(self.quarter // self.chip)]

    def slots(self):
        return [[self.at(0, 0)], [self.at(rs, 0) for rs in self.chips()], [self.at(rs, 1) for rs in self.chips()]]

    def norm(self, x, gain_ref, bias_ref, layer):
        return layer_norm(x, gain_ref[layer:layer + 1], bias_ref[layer:layer + 1], self.centring)

    def enter(self, blocks, gain_ref, bias_ref, gw_ref, gate_ref, x_ref):
        x = jnp.concatenate([b.reshape(self.area, self.c) for b in blocks], 0)
        normed = self.norm(x, gain_ref, bias_ref, 0)
        gate_ref[...] = jnp.tanh(mm(normed, gw_ref[0])).reshape(gate_ref.shape)
        x_ref[...] = x.astype(jnp.float32).reshape(x_ref.shape)
        return normed

    def edges(self, normed, w_ref, q, row_masks, column_mask):
        _, _, h, c = w_ref.shape
        p = mmt(normed, w_ref[0, q:q + 2].reshape(2 * h, c))
        shape = (normed.shape[0] // self.length, self.length, h)
        mask = row_masks[:, None, :] * column_mask[None]
        return gated(p[:, :h].reshape(shape), p[:, h:].reshape(shape) * mask)

    def turned(self, right):
        tile = right if right.shape[0] == self.chip else jnp.concatenate([right, right], 0)
        return jnp.swapaxes(tile, 0, 1)

    def triangle(self, left_ref, first, count, turned, tri_refs):
        h = left_ref.shape[2]
        low = lax.broadcasted_iota(jnp.int32, (self.chip, h), 0) < self.size
        acc = {}
        for m in range(self.length):
            ls = [left_ref[first + i, m:m + 1, :] for i in range(count)]
            for t, ref in turned.items():
                r = ref[m]
                for i in range(0, count, 2 if t == 0 else 1):
                    l = jnp.where(low, ls[i], ls[i + 1]) if t == 0 else ls[i]
                    acc[i, t] = acc[i, t] + l * r if m else l * r
        for (i, t), value in acc.items():
            ref, offset = tri_refs[t]
            ref[offset + ((first + i) // 2 if t == 0 else first + i)] = value

    def tiles(self, read, rows, slot):
        if slot == 0:
            parts = [read(pl.ds(i, rows // 2, stride=2), self.slots()[0][0]) for i in range(2)]
        else:
            parts = [read(pl.ds(0, rows), o) for o in self.slots()[slot]]
        tiles = jnp.concatenate(parts, 1)
        return tiles.reshape(tiles.shape[0] * tiles.shape[1], tiles.shape[2])

    def columns(self, refs):
        def one(ref, slot):
            return self.tiles(lambda rows, o: ref[rows, pl.ds(o, self.size), :], ref.shape[0], slot)

        return jnp.concatenate([one(ref, slot) for slot in range(3) for ref in refs], 0)

    def masks(self, mask_ref, row_mask_ref, slot):
        return self.tiles(
            lambda rows, o: row_mask_ref[rows][:, None, :] * mask_ref[pl.ds(o, self.size)][None], self.length, slot
        )

    def column_masks(self, mask_ref, slots):
        return jnp.concatenate([mask_ref[pl.ds(o, self.size)] for t in slots for o in self.slots()[t]], 0)


def keep(place, step, ref, w_ref):
    part = ref.shape[2]
    at = pl.multiple_of((place.chan ^ step) * part, part)
    w_ref[:, :, pl.ds(at, part), :] = ref[...] * jnp.bfloat16(0.5)


def early_kernel(counts, *refs):
    present_ref, ig_ref, ib_ref = refs[:3]
    sources = refs[3:9]
    gate_ref, x_ref, w_ref, mask_ref, row_mask_ref, gw_ref, fold_ref, shift_ref, normed_ref = refs[9:18]
    raw, sems = refs[18:24], refs[24]
    copies = [pltpu.make_async_copy(a, b, sems.at[i]) for i, (a, b) in enumerate(zip(sources, raw))]
    for copy in copies:
        copy.start()
    length, h = mask_ref.shape
    place = Place(counts, length, x_ref.shape[2])
    half = jnp.bfloat16(0.5)
    across = present_ref[...].astype(jnp.float32)
    square = (length, length)
    diagonal = lax.broadcasted_iota(jnp.int32, square, 0) == lax.broadcasted_iota(jnp.int32, square, 1)
    mask_ref[...] = mm(jnp.where(diagonal, across, 0.0).astype(jnp.bfloat16), jnp.ones((length, h), jnp.bfloat16))
    for i, where in enumerate(place.early + place.late):
        row_mask_ref[i * place.size:(i + 1) * place.size] = mask_ref[pl.ds(place.at(*where), place.size)]
    for copy in copies:
        copy.wait()
    pair_ref, projections_ref, gate_weight_ref, ow_ref, og_ref, ob_ref = raw
    gw_ref[...] = gate_weight_ref[...] * half
    keep(place, 0, projections_ref, w_ref)
    normed_ref[...] = place.enter([pair_ref[...]], ig_ref, ib_ref, gw_ref, gate_ref, x_ref)
    for layer in range(2):
        out = ow_ref[layer] * half
        folded = exact(place.centring.astype(jnp.float32) * og_ref[layer:layer + 1], out)
        high = folded.astype(jnp.bfloat16)
        fold_ref[layer, :h, :h] = place.centring
        fold_ref[layer, :h, h:] = high
        fold_ref[layer, h:, :h] = jnp.zeros((h, h), jnp.bfloat16)
        fold_ref[layer, h:, h:] = (folded - high.astype(jnp.float32)).astype(jnp.bfloat16)
        shift_ref[layer] = exact(jnp.broadcast_to(ob_ref[layer:layer + 1], (8, h)), out)


def arrived_kernel(counts, *refs):
    n = counts[0]
    blocks = refs[:n]
    ig_ref, ib_ref, gw_ref, own_ref, gate_ref, x_ref, normed_ref = refs[n:]
    place = Place(counts, x_ref.shape[1], x_ref.shape[2])
    normed_ref[0] = own_ref[...]
    normed = place.enter([b[...] for b in blocks], ig_ref, ib_ref, gw_ref, gate_ref, x_ref)
    normed_ref[1:] = normed.reshape(n, place.area, place.c)


def first_kernel(counts, ahead, *refs):
    n = counts[1] - 1
    weights = refs[:n]
    normed_ref, mask_ref, row_mask_ref, _, left_ref, turned_ref, tri_ref, w_ref = refs[n:]
    place = Place(counts, mask_ref.shape[0], normed_ref.shape[2])
    for i, ref in enumerate(weights):
        keep(place, i + 1, ref, w_ref)
    rows = left_ref.shape[0]
    mask = mask_ref[...]
    size = place.size
    wanted = jnp.concatenate([normed_ref[0], *[normed_ref[rs] for rs in place.chips()]], 0)
    right = place.edges(wanted, w_ref, 2, place.column_masks(mask_ref, (0, 1)), mask)
    turned_ref[0] = place.turned(right[:size])
    turned_ref[1] = place.turned(right[size:])
    every = normed_ref[...].reshape(-1, place.c)
    left_ref[...] = place.edges(every, w_ref, 0, row_mask_ref[:rows], mask)
    for i in range(0, ahead, size):
        place.triangle(
            left_ref, i, size, {0: turned_ref.at[0], 1: turned_ref.at[1]}, {0: (tri_ref, 0), 1: (tri_ref, ahead // 2)}
        )


def last_kernel(counts, ahead, *refs):
    n = counts[0] - 1
    blocks = refs[:n]
    (ig_ref, ib_ref, left_ref, turned_ref, tri_ref, gate0_ref, x0_ref, gate1_ref, x1_ref, normed_ref, w_ref, mask_ref,
     row_mask_ref, gw_ref, fold_ref, shift_ref, out_ref,
     gate2_ref, x2_ref, others_ref, late_ref, turned2_ref, tri0_ref, tri1_ref, tri2_ref, z_ref, l1_ref, r1_ref) = refs[n:]
    length, h = mask_ref.shape
    c = x0_ref.shape[2]
    place = Place(counts, length, c)
    size, chip, quarter = place.size, place.chip, place.quarter
    rows = left_ref.shape[0]
    mask = mask_ref[...]
    early_turned = {0: turned_ref.at[0], 1: turned_ref.at[1]}
    for i in range(ahead, rows, size):
        place.triangle(left_ref, i, size, early_turned, {0: (tri0_ref, -ahead // 2), 1: (tri1_ref, -ahead)})
    normed = place.enter([b[...] for b in blocks], ig_ref, ib_ref, gw_ref, gate2_ref, x2_ref)
    others_ref[0] = normed_ref[counts[0]]
    others_ref[1:] = normed.reshape(n, place.area, c)
    wanted = jnp.concatenate([others_ref[rs] for rs in place.chips()], 0)
    turned2_ref[...] = place.turned(place.edges(wanted, w_ref, 2, place.column_masks(mask_ref, (2,)), mask))
    late_ref[...] = place.edges(normed, w_ref, 0, row_mask_ref[rows:], mask)
    for i in range(0, rows, 2 * size):
        place.triangle(left_ref, i, min(2 * size, rows - i), {2: turned2_ref}, {2: (tri2_ref, 0)})
    late = late_ref.shape[0]
    for i in range(0, late, size):
        place.triangle(
            late_ref, i, size, {**early_turned, 2: turned2_ref},
            {0: (tri0_ref, (rows - ahead) // 2), 1: (tri1_ref, rows - ahead), 2: (tri2_ref, rows)},
        )

    def finish(tri, half_gate, residual, layer):
        both = tri.astype(jnp.bfloat16)
        both = mm(jnp.concatenate([both, both], 1), fold_ref[layer])
        centred = both[:, :h]
        spread = jnp.mean(centred * centred, axis=1, keepdims=True)
        update = both[:, h:] * lax.rsqrt(spread + epsilon) + shift_ref[layer, 0:1]
        return (residual + (update * half_gate + update)).astype(jnp.bfloat16)

    half_gate = place.columns((gate0_ref, gate1_ref, gate2_ref))
    residual = place.columns((x0_ref, x1_ref, x2_ref))
    tri = jnp.concatenate([tri_ref[:ahead // 2], tri0_ref[...], tri_ref[ahead // 2:], tri1_ref[...], tri2_ref[...]], 0)
    z = finish(tri.reshape(residual.shape[0], h), half_gate, residual, 0)
    area = length * size
    z_ref[...] = z[area:].astype(jnp.float32).reshape(2, length, chip, c)

    normed = place.norm(z, ig_ref, ib_ref, 1)
    p = mmt(normed[:area], w_ref[1, 0:2].reshape(2 * h, c))
    l1_ref[...] = gated(p[:, :h], p[:, h:] * place.masks(mask_ref, row_mask_ref, 0))
    p = mmt(normed[area:], w_ref[1, 2:4].reshape(2 * h, c))
    area = length * chip
    for t in (1, 2):
        at = slice((t - 1) * area, t * area)
        r1_ref[t - 1] = gated(p[at, :h], p[at, h:] * place.masks(mask_ref, row_mask_ref, t)).reshape(length, chip, h)
    mine = z_ref[:, :size].reshape(2 * size * chip, c)
    half_gate = jnp.tanh(mm(place.norm(mine.astype(jnp.bfloat16), ig_ref, ib_ref, 1), gw_ref[1]))

    acc = [jnp.zeros((chip, h), jnp.float32) for _ in range(2 * size)]
    for k in range(length):
        rs = [r1_ref[t, k] for t in range(2)]
        ls = [l1_ref[k * size + i:k * size + i + 1, :] for i in range(size)]
        acc = [acc[t * size + i] + ls[i] * rs[t] for t in range(2) for i in range(size)]
    z = finish(jnp.concatenate(acc, 0), half_gate, mine, 1).astype(jnp.float32).reshape(2, size, chip, c)
    even = jnp.where(place.sub == 0, z[0], z[1])
    odd = jnp.where(place.sub == 0, z[1], z[0])
    parts = [v[:, i * size:(i + 1) * size] for i in range(quarter // chip) for v in (even, odd)]
    out_ref[...] = jnp.concatenate(parts, 1).astype(jnp.bfloat16)


def in_vmem(value):
    return pltpu.with_memory_space_constraint(value, pltpu.VMEM)


def in_hbm(value):
    return pltpu.with_memory_space_constraint(value, pltpu.HBM)


VMEM = pl.BlockSpec(memory_space=pltpu.VMEM)
HBM = pl.BlockSpec(memory_space=pltpu.HBM)

AHEAD = 8


def gathered(
    pair, residue_mask, in_gain, in_bias, projections, gate_weight, out_gain, out_bias, out_weight
):
    rows_count, chan_count, sub_count = (lax.axis_size(a) for a in ("rows", "chan", "sub"))
    size, length, c = pair.shape
    h = out_weight.shape[1]
    chip, area = size * sub_count, size * length
    counts = (rows_count, chan_count, sub_count, size)
    turned = jnp.swapaxes(projections, 2, 3)
    hops = tuple(range(1, rows_count))
    far, near = {}, {}
    for rs in hops:
        far[rs] = swap(pair, "rows", rs)
    near[0] = swap(pair, "sub", 1)
    weights = [swap(turned, "chan", i) for i in range(1, chan_count)]
    for rs in hops:
        near[rs] = swap(far[rs], "sub", 1)

    def f32(*shape):
        return pltpu.VMEM(shape, jnp.float32)

    def bf16(*shape):
        return pltpu.VMEM(shape, jnp.bfloat16)

    def call(kernel, near, far, out_shape, scratch=(), aliases={}, rows=0, mib=8):
        return pl.pallas_call(
            kernel,
            out_shape=out_shape,
            in_specs=[VMEM] * len(near) + [HBM] * len(far),
            out_specs=jax.tree.map(lambda _: VMEM, out_shape),
            scratch_shapes=[
                *scratch,
                *[pltpu.VMEM(o.shape, o.dtype) for o in far],
                *([pltpu.SemaphoreType.DMA((len(far),))] if far else []),
            ],
            input_output_aliases=aliases,
            compiler_params=pltpu.CompilerParams(vmem_limit_bytes=mib << 20),
            cost_estimate=pl.CostEstimate(flops=rows * c * c * 16, bytes_accessed=0, transcendentals=0),
        )(*[in_vmem(o) for o in near], *[in_hbm(o) for o in far])

    gate0, x0, w, mask, row_mask, gw, fold, shift, own = call(
        functools.partial(early_kernel, counts),
        [residue_mask[None], in_gain, in_bias],
        [pair, turned, gate_weight, out_weight, out_gain, out_bias],
        [
            f32(size, length, c),
            f32(size, length, c),
            bf16(2, 4, h, c),
            f32(length, h),
            f32(length, h),
            bf16(2, c, c),
            bf16(2, 2 * h, h + c),
            f32(2, 8, c),
            bf16(area, c),
        ],
        rows=length * length,
    )
    gate1, x1, normed = call(
        functools.partial(arrived_kernel, counts),
        [*[far[rs] for rs in hops], near[0], in_gain, in_bias, gw, own],
        [],
        [
            f32(rows_count * size, length, c),
            f32(rows_count * size, length, c),
            bf16(rows_count + 1, area, c),
        ],
        rows=length * length,
    )
    early = (rows_count + 1) * size
    late = length - early
    operands = [*weights, normed, mask, row_mask, w]
    left, right, tri, w = call(
        functools.partial(first_kernel, counts, AHEAD),
        operands,
        [],
        [f32(early, length, h), f32(2, length, chip, h), f32(AHEAD // 2 + AHEAD, chip, h), bf16(2, 4, h, c)],
        aliases={len(operands) - 1: 3},
        rows=length * length,
    )
    operands = [
        *[near[rs] for rs in hops], in_gain, in_bias, left, right, tri, gate0, x0, gate1, x1, normed, w, mask, row_mask,
        gw, fold, shift,
    ]
    return call(
        functools.partial(last_kernel, counts, AHEAD),
        operands,
        [],
        jax.ShapeDtypeStruct((size, length // chan_count, c), jnp.bfloat16),
        scratch=[
            f32(late, length, c),
            f32(late, length, c),
            bf16(rows_count, area, c),
            f32(late, length, h),
            f32(length, chip, h),
            f32((length - AHEAD) // 2, chip, h),
            f32(length - AHEAD, chip, h),
            f32(length, chip, h),
            f32(2, length, chip, c),
            f32(length * size, h),
            f32(2, length, chip, h),
        ],
        rows=1,
        mib=16,
    )


def solution(mesh):
    def body(pair, *rest):
        size, length, c = pair.shape
        small = 2 * length * length * c <= GATHER_LIMIT
        fits = (
            mesh.shape["sub"] == 2
            and mesh.shape["rows"] & (mesh.shape["rows"] - 1) == 0
            and size * 2 == 8
            and length == 16 * mesh.shape["chan"]
        )
        if not (small and fits):
            return shards(pair, *rest)
        return gathered(pair, *rest)

    placed = (
        P(("crops", "rows", "sub"), None, None),
        P("crops"),
        P(),
        P(),
        P(None, None, None, "chan"),
        P(),
        P(),
        P(),
        P(),
    )
    step = jax.shard_map(
        body,
        mesh=mesh,
        in_specs=placed,
        out_specs=P(("crops", "rows", "sub"), "chan", None),
        check_vma=False,
    )
    if 8 * mesh.shape["rows"] != 16 * mesh.shape["chan"]:
        return step
    return step
```

```python
import functools

import jax
import jax.numpy as jnp
from jax import lax
from jax.experimental import pallas as pl
from jax.experimental.pallas import tpu as pltpu
from jax.sharding import PartitionSpec as P


epsilon = 1e-05


GATHER_LIMIT = 1 << 20


def normalize(values, reduce_axis):
    centre = jnp.mean(values, axis=reduce_axis, keepdims=True)
    centred = values - centre
    spread = jnp.mean(centred * centred, axis=reduce_axis, keepdims=True)
    return centred * lax.rsqrt(spread + epsilon)


def shards(
    pair, residue_mask, in_gain, in_bias, projections, gate_weight, out_gain, out_bias, out_weight
):
    rows_block = pair.shape[0]
    length = pair.shape[1]
    chan_count = lax.axis_size("chan")
    chan_index = lax.axis_index("chan")
    quarter = length // chan_count
    row_start = lax.axis_index(("rows", "sub")) * rows_block
    mask_float = residue_mask.astype(jnp.float32)
    own_mask = lax.dynamic_slice_in_dim(mask_float, row_start, rows_block)
    pair_mask = own_mask[None, :, None] * mask_float[None, None, :]

    def project(full_rows, layer_index):
        normed = (
            normalize(full_rows.astype(jnp.float32), 2) * in_gain[layer_index]
            + in_bias[layer_index]
        ).astype(jnp.bfloat16)
        projected = jnp.einsum(
            "ikc,qch->qhik", normed, projections[layer_index], preferred_element_type=jnp.float32
        )
        left_edges = (jax.nn.sigmoid(projected[0]) * projected[1] * pair_mask).astype(jnp.bfloat16)
        right_edges = (jax.nn.sigmoid(projected[2]) * projected[3] * pair_mask).astype(jnp.bfloat16)
        return (normed, left_edges, right_edges)

    def finish(triangle, normed, residual, layer_index):
        gathered = lax.all_to_all(triangle, "chan", split_axis=2, concat_axis=0, tiled=True)
        whole_float = gathered.astype(jnp.float32)
        scaled = (
            normalize(whole_float, 0) * out_gain[layer_index][:, None, None]
            + out_bias[layer_index][:, None, None]
        ).astype(jnp.bfloat16)
        update = jnp.einsum(
            "hij,hc->ijc", scaled, out_weight[layer_index], preferred_element_type=jnp.float32
        )
        normed_part = lax.dynamic_slice_in_dim(normed, chan_index * quarter, quarter, 1)
        gating = jax.nn.sigmoid(
            jnp.einsum(
                "ijc,cd->ijd",
                normed_part,
                gate_weight[layer_index],
                preferred_element_type=jnp.float32,
            )
        )
        return (residual.astype(jnp.float32) + gating * update).astype(jnp.bfloat16)

    normed, left_edges, right_edges = project(pair, 0)
    triangle = jnp.einsum(
        "hik,hjk->hij",
        left_edges,
        lax.all_gather(right_edges, ("rows", "sub"), axis=1, tiled=True),
        preferred_element_type=jnp.float32,
    ).astype(jnp.bfloat16)
    own_quarter = lax.dynamic_slice_in_dim(pair, chan_index * quarter, quarter, 1)
    layer_one = finish(triangle, normed, own_quarter, 0)
    full_rows = lax.all_gather(layer_one, "chan", axis=1, tiled=True)
    normed, left_edges, right_edges = project(full_rows, 1)
    left_cols, right_cols = (
        lax.all_to_all(left_edges, ("rows", "sub"), split_axis=2, concat_axis=1, tiled=True),
        lax.all_to_all(right_edges, ("rows", "sub"), split_axis=2, concat_axis=1, tiled=True),
    )
    triangle = jnp.einsum(
        "hki,hkj->hij",
        left_cols,
        lax.all_gather(right_cols, ("rows", "sub"), axis=2, tiled=True),
        preferred_element_type=jnp.float32,
    )
    return finish(triangle.astype(jnp.bfloat16), normed, layer_one, 1)


def swap(value, axis, step):
    count = lax.axis_size(axis)
    return lax.ppermute(value, axis, [(i, i ^ step) for i in range(count)])


def mm(a, b):
    return jnp.dot(a, b, preferred_element_type=jnp.float32)


def mmt(a, b):
    return lax.dot_general(a, b, (((1,), (1,)), ((), ())), preferred_element_type=jnp.float32)


def constants(c):
    diagonal = lax.broadcasted_iota(jnp.int32, (c, c), 0) == lax.broadcasted_iota(jnp.int32, (c, c), 1)
    return jnp.where(diagonal, 1.0 - 1.0 / c, -1.0 / c).astype(jnp.bfloat16)


def exact(a, b):
    total = 0.0
    for _ in range(3):
        piece = a.astype(jnp.bfloat16)
        total = total + mm(piece, b)
        a = a - piece.astype(jnp.float32)
    return total


def layer_norm(values, gain, bias, centring):
    centred = mm(values, centring)
    spread = jnp.mean(centred * centred, axis=1, keepdims=True)
    return (centred * lax.rsqrt(spread + epsilon) * gain + bias).astype(jnp.bfloat16)


def gated(half_gate, half_value):
    return half_value * jnp.tanh(half_gate) + half_value


class Place:
    def __init__(self, counts, length, c):
        self.rows_count, self.chan_count, self.sub_count, self.size = counts
        self.length, self.c = length, c
        self.row = lax.axis_index("rows")
        self.chan = lax.axis_index("chan")
        self.sub = lax.axis_index("sub")
        self.chip = self.size * self.sub_count
        self.quarter = length // self.chan_count
        self.area = self.size * length
        self.centring = constants(c)
        hops = range(1, self.rows_count)
        self.early = [(0, 0), *[(rs, 0) for rs in hops], (0, 1)]
        self.late = [(rs, 1) for rs in hops]

    def at(self, rs, ss):
        return ((self.row ^ rs) * self.sub_count + (self.sub ^ ss)) * self.size

    def chips(self):
        return [(self.chan * (self.quarter // self.chip) + i) ^ self.row for i in range(self.quarter // self.chip)]

    def slots(self):
        return [[self.at(0, 0)], [self.at(rs, 0) for rs in self.chips()], [self.at(rs, 1) for rs in self.chips()]]

    def norm(self, x, gain_ref, bias_ref, layer):
        return layer_norm(x, gain_ref[layer:layer + 1], bias_ref[layer:layer + 1], self.centring)

    def enter(self, blocks, gain_ref, bias_ref, gw_ref, gate_ref, x_ref):
        x = jnp.concatenate([b.reshape(self.area, self.c) for b in blocks], 0)
        normed = self.norm(x, gain_ref, bias_ref, 0)
        gate_ref[...] = jnp.tanh(mm(normed, gw_ref[0])).reshape(gate_ref.shape)
        x_ref[...] = x.astype(jnp.float32).reshape(x_ref.shape)
        return normed

    def edges(self, normed, w_ref, q, mask):
        _, _, h, c = w_ref.shape
        p = mmt(normed, w_ref[0, q:q + 2].reshape(2 * h, c))
        shape = (normed.shape[0] // self.length, self.length, h)
        return gated(p[:, :h].reshape(shape), p[:, h:].reshape(shape) * mask)

    def turned(self, right):
        tile = right if right.shape[0] == self.chip else jnp.concatenate([right, right], 0)
        return jnp.swapaxes(tile, 0, 1)

    def triangle(self, left_ref, first, count, turned, tri_refs):
        h = left_ref.shape[2]
        low = lax.broadcasted_iota(jnp.int32, (self.chip, h), 0) < self.size
        acc = {}
        for m in range(self.length):
            ls = [left_ref[first + i, m:m + 1, :] for i in range(count)]
            for t, ref in turned.items():
                r = ref[m]
                for i in range(0, count, 2 if t == 0 else 1):
                    l = jnp.where(low, ls[i], ls[i + 1]) if t == 0 else ls[i]
                    acc[i, t] = acc[i, t] + l * r if m else l * r
        for (i, t), value in acc.items():
            ref, offset = tri_refs[t]
            ref[offset + ((first + i) // 2 if t == 0 else first + i)] = value

    def tiles(self, read, rows, slot):
        if slot == 0:
            parts = [read(pl.ds(i, rows // 2, stride=2), self.slots()[0][0]) for i in range(2)]
        else:
            parts = [read(pl.ds(0, rows), o) for o in self.slots()[slot]]
        tiles = jnp.concatenate(parts, 1)
        return tiles.reshape(tiles.shape[0] * tiles.shape[1], tiles.shape[2])

    def columns(self, refs):
        def one(ref, slot):
            return self.tiles(lambda rows, o: ref[rows, pl.ds(o, self.size), :], ref.shape[0], slot)

        return jnp.concatenate([one(ref, slot) for slot in range(3) for ref in refs], 0)

    def masks(self, mask_ref, row_mask_ref, slot):
        return self.tiles(
            lambda rows, o: row_mask_ref[rows][:, None, :] * mask_ref[pl.ds(o, self.size)][None], self.length, slot
        )

    def column_masks(self, mask_ref, slots):
        return jnp.concatenate([mask_ref[pl.ds(o, self.size)] for t in slots for o in self.slots()[t]], 0)


def keep(place, step, ref, w_ref):
    part = ref.shape[2]
    at = pl.multiple_of((place.chan ^ step) * part, part)
    w_ref[:, :, pl.ds(at, part), :] = ref[...] * jnp.bfloat16(0.5)


def early_kernel(counts, *refs):
    present_ref, ig_ref, ib_ref = refs[:3]
    sources = refs[3:9]
    gate_ref, x_ref, w_ref, mask_ref, row_mask_ref, gw_ref, fold_ref, shift_ref, normed_ref = refs[9:18]
    raw, sems = refs[18:24], refs[24]
    copies = [pltpu.make_async_copy(a, b, sems.at[i]) for i, (a, b) in enumerate(zip(sources, raw))]
    for copy in copies:
        copy.start()
    length, h = mask_ref.shape
    place = Place(counts, length, x_ref.shape[2])
    half = jnp.bfloat16(0.5)
    across = present_ref[...].astype(jnp.float32)
    square = (length, length)
    diagonal = lax.broadcasted_iota(jnp.int32, square, 0) == lax.broadcasted_iota(jnp.int32, square, 1)
    mask_ref[...] = mm(jnp.where(diagonal, across, 0.0).astype(jnp.bfloat16), jnp.ones((length, h), jnp.bfloat16))
    for i, where in enumerate(place.early + place.late):
        row_mask_ref[i * place.size:(i + 1) * place.size] = mask_ref[pl.ds(place.at(*where), place.size)]
    for copy in copies:
        copy.wait()
    pair_ref, projections_ref, gate_weight_ref, ow_ref, og_ref, ob_ref = raw
    gw_ref[...] = gate_weight_ref[...] * half
    keep(place, 0, projections_ref, w_ref)
    normed_ref[...] = place.enter([pair_ref[...]], ig_ref, ib_ref, gw_ref, gate_ref, x_ref)
    for layer in range(2):
        out = ow_ref[layer] * half
        folded = exact(place.centring.astype(jnp.float32) * og_ref[layer:layer + 1], out)
        high = folded.astype(jnp.bfloat16)
        fold_ref[layer, :h, :h] = place.centring
        fold_ref[layer, :h, h:] = high
        fold_ref[layer, h:, :h] = jnp.zeros((h, h), jnp.bfloat16)
        fold_ref[layer, h:, h:] = (folded - high.astype(jnp.float32)).astype(jnp.bfloat16)
        shift_ref[layer] = exact(jnp.broadcast_to(ob_ref[layer:layer + 1], (8, h)), out)


def arrived_kernel(counts, *refs):
    n = counts[0]
    blocks = refs[:n]
    ig_ref, ib_ref, gw_ref, own_ref, gate_ref, x_ref, normed_ref = refs[n:]
    place = Place(counts, x_ref.shape[1], x_ref.shape[2])
    normed_ref[0] = own_ref[...]
    normed = place.enter([b[...] for b in blocks], ig_ref, ib_ref, gw_ref, gate_ref, x_ref)
    normed_ref[1:] = normed.reshape(n, place.area, place.c)


def first_kernel(counts, ahead, *refs):
    n = counts[1] - 1
    weights = refs[:n]
    normed_ref, mask_ref, row_mask_ref, _, left_ref, turned_ref, tri_ref, w_ref = refs[n:]
    place = Place(counts, mask_ref.shape[0], normed_ref.shape[2])
    for i, ref in enumerate(weights):
        keep(place, i + 1, ref, w_ref)
    rows = left_ref.shape[0]
    mask = mask_ref[...]
    size = place.size
    wanted = jnp.concatenate([normed_ref[0], *[normed_ref[rs] for rs in place.chips()]], 0)
    right = place.edges(wanted, w_ref, 2, place.column_masks(mask_ref, (0, 1))[:, None, :] * mask[None])
    turned_ref[0] = place.turned(right[:size])
    turned_ref[1] = place.turned(right[size:])
    every = normed_ref[...].reshape(-1, place.c)
    left_ref[...] = place.edges(every, w_ref, 0, row_mask_ref[:rows][:, None, :])
    for i in range(0, ahead, size):
        place.triangle(
            left_ref, i, size, {0: turned_ref.at[0], 1: turned_ref.at[1]}, {0: (tri_ref, 0), 1: (tri_ref, ahead // 2)}
        )


def last_kernel(counts, ahead, *refs):
    n = counts[0] - 1
    blocks = refs[:n]
    (ig_ref, ib_ref, left_ref, turned_ref, tri_ref, gate0_ref, x0_ref, gate1_ref, x1_ref, normed_ref, w_ref, mask_ref,
     row_mask_ref, gw_ref, fold_ref, shift_ref, out_ref,
     gate2_ref, x2_ref, others_ref, late_ref, turned2_ref, tri0_ref, tri1_ref, tri2_ref, l1_ref, r1_ref) = refs[n:]
    length, h = mask_ref.shape
    c = x0_ref.shape[2]
    place = Place(counts, length, c)
    size, chip, quarter = place.size, place.chip, place.quarter
    rows = left_ref.shape[0]
    mask = mask_ref[...]
    early_turned = {0: turned_ref.at[0], 1: turned_ref.at[1]}
    for i in range(ahead, rows, size):
        place.triangle(left_ref, i, size, early_turned, {0: (tri0_ref, -ahead // 2), 1: (tri1_ref, -ahead)})
    normed = place.enter([b[...] for b in blocks], ig_ref, ib_ref, gw_ref, gate2_ref, x2_ref)
    others_ref[0] = normed_ref[counts[0]]
    others_ref[1:] = normed.reshape(n, place.area, c)
    wanted = jnp.concatenate([others_ref[rs] for rs in place.chips()], 0)
    turned2_ref[...] = place.turned(
        place.edges(wanted, w_ref, 2, place.column_masks(mask_ref, (2,))[:, None, :] * mask[None])
    )
    late_ref[...] = place.edges(normed, w_ref, 0, row_mask_ref[rows:][:, None, :])
    for i in range(0, rows, 2 * size):
        place.triangle(left_ref, i, min(2 * size, rows - i), {2: turned2_ref}, {2: (tri2_ref, 0)})
    late = late_ref.shape[0]
    for i in range(0, late, size):
        place.triangle(
            late_ref, i, size, {**early_turned, 2: turned2_ref},
            {0: (tri0_ref, (rows - ahead) // 2), 1: (tri1_ref, rows - ahead), 2: (tri2_ref, rows)},
        )

    def finish(tri, half_gate, residual, layer):
        both = tri.astype(jnp.bfloat16)
        both = mm(jnp.concatenate([both, both], 1), fold_ref[layer])
        centred = both[:, :h]
        spread = jnp.mean(centred * centred, axis=1, keepdims=True)
        update = both[:, h:] * lax.rsqrt(spread + epsilon) + shift_ref[layer, 0:1]
        return (residual + (update * half_gate + update)).astype(jnp.bfloat16)

    half_gate = place.columns((gate0_ref, gate1_ref, gate2_ref))
    residual = place.columns((x0_ref, x1_ref, x2_ref))
    tri = jnp.concatenate([tri_ref[:ahead // 2], tri0_ref[...], tri_ref[ahead // 2:], tri1_ref[...], tri2_ref[...]], 0)
    z = finish(tri.reshape(residual.shape[0], h), half_gate, residual, 0)
    area = length * size

    normed = place.norm(z, ig_ref, ib_ref, 1)
    starts = [area + t * length * chip for t in range(2)]
    mine = jnp.concatenate([z[a:a + size * chip] for a in starts], 0).astype(jnp.float32)
    mine_normed = jnp.concatenate([normed[a:a + size * chip] for a in starts], 0)
    p = mmt(normed[:area], w_ref[1, 0:2].reshape(2 * h, c))
    l1_ref[...] = gated(p[:, :h], p[:, h:] * place.masks(mask_ref, row_mask_ref, 0))
    p = mmt(normed[area:], w_ref[1, 2:4].reshape(2 * h, c))
    area = length * chip
    for t in (1, 2):
        at = slice((t - 1) * area, t * area)
        columns = place.column_masks(mask_ref, (t,))[None]
        shape = (length, chip, h)
        r1_ref[t - 1] = gated(p[at, :h].reshape(shape), p[at, h:].reshape(shape) * columns)
    half_gate = jnp.tanh(mm(mine_normed, gw_ref[1]))

    acc = [jnp.zeros((chip, h), jnp.float32) for _ in range(2 * size)]
    for k in range(length):
        rs = [r1_ref[t, k] for t in range(2)]
        ls = [l1_ref[k * size + i:k * size + i + 1, :] for i in range(size)]
        acc = [acc[t * size + i] + ls[i] * rs[t] for t in range(2) for i in range(size)]
    z = finish(jnp.concatenate(acc, 0), half_gate, mine, 1).astype(jnp.float32).reshape(2, size, chip, c)
    even = jnp.where(place.sub == 0, z[0], z[1])
    odd = jnp.where(place.sub == 0, z[1], z[0])
    parts = [v[:, i * size:(i + 1) * size] for i in range(quarter // chip) for v in (even, odd)]
    out_ref[...] = jnp.concatenate(parts, 1).astype(jnp.bfloat16)


def in_vmem(value):
    return pltpu.with_memory_space_constraint(value, pltpu.VMEM)


def in_hbm(value):
    return pltpu.with_memory_space_constraint(value, pltpu.HBM)


VMEM = pl.BlockSpec(memory_space=pltpu.VMEM)
HBM = pl.BlockSpec(memory_space=pltpu.HBM)

AHEAD = 12


def gathered(
    pair, residue_mask, in_gain, in_bias, projections, gate_weight, out_gain, out_bias, out_weight
):
    rows_count, chan_count, sub_count = (lax.axis_size(a) for a in ("rows", "chan", "sub"))
    size, length, c = pair.shape
    h = out_weight.shape[1]
    chip, area = size * sub_count, size * length
    counts = (rows_count, chan_count, sub_count, size)
    turned = jnp.swapaxes(projections, 2, 3)
    hops = tuple(range(1, rows_count))
    far, near = {}, {}
    for rs in hops:
        far[rs] = swap(pair, "rows", rs)
    near[0] = swap(pair, "sub", 1)
    weights = [swap(turned, "chan", i) for i in range(1, chan_count)]
    for rs in hops:
        near[rs] = swap(far[rs], "sub", 1)

    def f32(*shape):
        return pltpu.VMEM(shape, jnp.float32)

    def bf16(*shape):
        return pltpu.VMEM(shape, jnp.bfloat16)

    def call(kernel, near, far, out_shape, scratch=(), aliases={}, rows=0, mib=8):
        return pl.pallas_call(
            kernel,
            out_shape=out_shape,
            in_specs=[VMEM] * len(near) + [HBM] * len(far),
            out_specs=jax.tree.map(lambda _: VMEM, out_shape),
            scratch_shapes=[
                *scratch,
                *[pltpu.VMEM(o.shape, o.dtype) for o in far],
                *([pltpu.SemaphoreType.DMA((len(far),))] if far else []),
            ],
            input_output_aliases=aliases,
            compiler_params=pltpu.CompilerParams(vmem_limit_bytes=mib << 20),
            cost_estimate=pl.CostEstimate(flops=rows * c * c * 16, bytes_accessed=0, transcendentals=0),
        )(*[in_vmem(o) for o in near], *[in_hbm(o) for o in far])

    gate0, x0, w, mask, row_mask, gw, fold, shift, own = call(
        functools.partial(early_kernel, counts),
        [residue_mask[None], in_gain, in_bias],
        [pair, turned, gate_weight, out_weight, out_gain, out_bias],
        [
            f32(size, length, c),
            f32(size, length, c),
            bf16(2, 4, h, c),
            f32(length, h),
            f32(length, h),
            bf16(2, c, c),
            bf16(2, 2 * h, h + c),
            f32(2, 8, c),
            bf16(area, c),
        ],
        rows=length * length,
    )
    gate1, x1, normed = call(
        functools.partial(arrived_kernel, counts),
        [*[far[rs] for rs in hops], near[0], in_gain, in_bias, gw, own],
        [],
        [
            f32(rows_count * size, length, c),
            f32(rows_count * size, length, c),
            bf16(rows_count + 1, area, c),
        ],
        rows=length * length,
    )
    early = (rows_count + 1) * size
    late = length - early
    operands = [*weights, normed, mask, row_mask, w]
    left, right, tri, w = call(
        functools.partial(first_kernel, counts, AHEAD),
        operands,
        [],
        [f32(early, length, h), f32(2, length, chip, h), f32(AHEAD // 2 + AHEAD, chip, h), bf16(2, 4, h, c)],
        aliases={len(operands) - 1: 3},
        rows=length * length,
    )
    operands = [
        *[near[rs] for rs in hops], in_gain, in_bias, left, right, tri, gate0, x0, gate1, x1, normed, w, mask, row_mask,
        gw, fold, shift,
    ]
    return call(
        functools.partial(last_kernel, counts, AHEAD),
        operands,
        [],
        jax.ShapeDtypeStruct((size, length // chan_count, c), jnp.bfloat16),
        scratch=[
            f32(late, length, c),
            f32(late, length, c),
            bf16(rows_count, area, c),
            f32(late, length, h),
            f32(length, chip, h),
            f32((length - AHEAD) // 2, chip, h),
            f32(length - AHEAD, chip, h),
            f32(length, chip, h),
            f32(length * size, h),
            f32(2, length, chip, h),
        ],
        rows=1,
        mib=16,
    )


def solution(mesh):
    def body(pair, *rest):
        size, length, c = pair.shape
        small = 2 * length * length * c <= GATHER_LIMIT
        fits = (
            mesh.shape["sub"] == 2
            and mesh.shape["rows"] & (mesh.shape["rows"] - 1) == 0
            and size * 2 == 8
            and length == 16 * mesh.shape["chan"]
        )
        if not (small and fits):
            return shards(pair, *rest)
        return gathered(pair, *rest)

    placed = (
        P(("crops", "rows", "sub"), None, None),
        P("crops"),
        P(),
        P(),
        P(None, None, None, "chan"),
        P(),
        P(),
        P(),
        P(),
    )
    step = jax.shard_map(
        body,
        mesh=mesh,
        in_specs=placed,
        out_specs=P(("crops", "rows", "sub"), "chan", None),
        check_vma=False,
    )
    if 8 * mesh.shape["rows"] != 16 * mesh.shape["chan"]:
        return step
    return step
```

```python
import functools

import jax
import jax.numpy as jnp
from jax import lax
from jax.experimental import pallas as pl
from jax.experimental.pallas import tpu as pltpu
from jax.sharding import PartitionSpec as P


epsilon = 1e-05


GATHER_LIMIT = 1 << 20


def normalize(values, reduce_axis):
    centre = jnp.mean(values, axis=reduce_axis, keepdims=True)
    centred = values - centre
    spread = jnp.mean(centred * centred, axis=reduce_axis, keepdims=True)
    return centred * lax.rsqrt(spread + epsilon)


def shards(
    pair, residue_mask, in_gain, in_bias, projections, gate_weight, out_gain, out_bias, out_weight
):
    rows_block = pair.shape[0]
    length = pair.shape[1]
    chan_count = lax.axis_size("chan")
    chan_index = lax.axis_index("chan")
    quarter = length // chan_count
    row_start = lax.axis_index(("rows", "sub")) * rows_block
    mask_float = residue_mask.astype(jnp.float32)
    own_mask = lax.dynamic_slice_in_dim(mask_float, row_start, rows_block)
    pair_mask = own_mask[None, :, None] * mask_float[None, None, :]

    def project(full_rows, layer_index):
        normed = (
            normalize(full_rows.astype(jnp.float32), 2) * in_gain[layer_index]
            + in_bias[layer_index]
        ).astype(jnp.bfloat16)
        projected = jnp.einsum(
            "ikc,qch->qhik", normed, projections[layer_index], preferred_element_type=jnp.float32
        )
        left_edges = (jax.nn.sigmoid(projected[0]) * projected[1] * pair_mask).astype(jnp.bfloat16)
        right_edges = (jax.nn.sigmoid(projected[2]) * projected[3] * pair_mask).astype(jnp.bfloat16)
        return (normed, left_edges, right_edges)

    def finish(triangle, normed, residual, layer_index):
        gathered = lax.all_to_all(triangle, "chan", split_axis=2, concat_axis=0, tiled=True)
        whole_float = gathered.astype(jnp.float32)
        scaled = (
            normalize(whole_float, 0) * out_gain[layer_index][:, None, None]
            + out_bias[layer_index][:, None, None]
        ).astype(jnp.bfloat16)
        update = jnp.einsum(
            "hij,hc->ijc", scaled, out_weight[layer_index], preferred_element_type=jnp.float32
        )
        normed_part = lax.dynamic_slice_in_dim(normed, chan_index * quarter, quarter, 1)
        gating = jax.nn.sigmoid(
            jnp.einsum(
                "ijc,cd->ijd",
                normed_part,
                gate_weight[layer_index],
                preferred_element_type=jnp.float32,
            )
        )
        return (residual.astype(jnp.float32) + gating * update).astype(jnp.bfloat16)

    normed, left_edges, right_edges = project(pair, 0)
    triangle = jnp.einsum(
        "hik,hjk->hij",
        left_edges,
        lax.all_gather(right_edges, ("rows", "sub"), axis=1, tiled=True),
        preferred_element_type=jnp.float32,
    ).astype(jnp.bfloat16)
    own_quarter = lax.dynamic_slice_in_dim(pair, chan_index * quarter, quarter, 1)
    layer_one = finish(triangle, normed, own_quarter, 0)
    full_rows = lax.all_gather(layer_one, "chan", axis=1, tiled=True)
    normed, left_edges, right_edges = project(full_rows, 1)
    left_cols, right_cols = (
        lax.all_to_all(left_edges, ("rows", "sub"), split_axis=2, concat_axis=1, tiled=True),
        lax.all_to_all(right_edges, ("rows", "sub"), split_axis=2, concat_axis=1, tiled=True),
    )
    triangle = jnp.einsum(
        "hki,hkj->hij",
        left_cols,
        lax.all_gather(right_cols, ("rows", "sub"), axis=2, tiled=True),
        preferred_element_type=jnp.float32,
    )
    return finish(triangle.astype(jnp.bfloat16), normed, layer_one, 1)


def swap(value, axis, step):
    count = lax.axis_size(axis)
    return lax.ppermute(value, axis, [(i, i ^ step) for i in range(count)])


def mm(a, b):
    return jnp.dot(a, b, preferred_element_type=jnp.float32)


def mmt(a, b):
    return lax.dot_general(a, b, (((1,), (1,)), ((), ())), preferred_element_type=jnp.float32)


def constants(c):
    diagonal = lax.broadcasted_iota(jnp.int32, (c, c), 0) == lax.broadcasted_iota(jnp.int32, (c, c), 1)
    return jnp.where(diagonal, 1.0 - 1.0 / c, -1.0 / c).astype(jnp.bfloat16)


def exact(a, b):
    total = 0.0
    for _ in range(3):
        piece = a.astype(jnp.bfloat16)
        total = total + mm(piece, b)
        a = a - piece.astype(jnp.float32)
    return total


def layer_norm(values, gain, bias, centring):
    centred = mm(values, centring)
    spread = jnp.mean(centred * centred, axis=1, keepdims=True)
    return (centred * lax.rsqrt(spread + epsilon) * gain + bias).astype(jnp.bfloat16)


def gated(half_gate, half_value):
    return half_value * jnp.tanh(half_gate) + half_value


class Place:
    def __init__(self, counts, length, c):
        self.rows_count, self.chan_count, self.sub_count, self.size = counts
        self.length, self.c = length, c
        self.row = lax.axis_index("rows")
        self.chan = lax.axis_index("chan")
        self.sub = lax.axis_index("sub")
        self.chip = self.size * self.sub_count
        self.quarter = length // self.chan_count
        self.area = self.size * length
        self.centring = constants(c)
        hops = range(1, self.rows_count)
        self.early = [(0, 0), *[(rs, 0) for rs in hops], (0, 1)]
        self.late = [(rs, 1) for rs in hops]

    def at(self, rs, ss):
        return ((self.row ^ rs) * self.sub_count + (self.sub ^ ss)) * self.size

    def chips(self):
        return [(self.chan * (self.quarter // self.chip) + i) ^ self.row for i in range(self.quarter // self.chip)]

    def slots(self):
        return [[self.at(0, 0)], [self.at(rs, 0) for rs in self.chips()], [self.at(rs, 1) for rs in self.chips()]]

    def norm(self, x, gain_ref, bias_ref, layer):
        return layer_norm(x, gain_ref[layer:layer + 1], bias_ref[layer:layer + 1], self.centring)

    def enter(self, blocks, gain_ref, bias_ref, gw_ref, gate_ref, x_ref):
        x = jnp.concatenate([b.reshape(self.area, self.c) for b in blocks], 0)
        normed = self.norm(x, gain_ref, bias_ref, 0)
        gate_ref[...] = (1.0 + jnp.tanh(mm(normed, gw_ref[0]))).reshape(gate_ref.shape)
        x_ref[...] = x.astype(jnp.float32).reshape(x_ref.shape)
        return normed

    def edges(self, normed, w_ref, q, mask):
        _, _, h, c = w_ref.shape
        p = mmt(normed, w_ref[0, q:q + 2].reshape(2 * h, c))
        shape = (normed.shape[0] // self.length, self.length, h)
        return gated(p[:, :h].reshape(shape), p[:, h:].reshape(shape) * mask)

    def turned(self, right):
        tile = right if right.shape[0] == self.chip else jnp.concatenate([right, right], 0)
        return jnp.swapaxes(tile, 0, 1)

    def triangle(self, left_ref, first, count, turned, tri_refs):
        h = left_ref.shape[2]
        low = lax.broadcasted_iota(jnp.int32, (self.chip, h), 0) < self.size
        acc = {}
        for m in range(self.length):
            ls = [left_ref[first + i, m:m + 1, :] for i in range(count)]
            for t, ref in turned.items():
                r = ref[m]
                for i in range(0, count, 2 if t == 0 else 1):
                    l = jnp.where(low, ls[i], ls[i + 1]) if t == 0 else ls[i]
                    acc[i, t] = acc[i, t] + l * r if m else l * r
        for (i, t), value in acc.items():
            ref, offset = tri_refs[t]
            ref[offset + ((first + i) // 2 if t == 0 else first + i)] = value

    def tiles(self, read, rows, slot):
        if slot == 0:
            parts = [read(pl.ds(i, rows // 2, stride=2), self.slots()[0][0]) for i in range(2)]
        else:
            parts = [read(pl.ds(0, rows), o) for o in self.slots()[slot]]
        tiles = jnp.concatenate(parts, 1)
        return tiles.reshape(tiles.shape[0] * tiles.shape[1], tiles.shape[2])

    def columns(self, refs):
        def one(ref, slot):
            return self.tiles(lambda rows, o: ref[rows, pl.ds(o, self.size), :], ref.shape[0], slot)

        return jnp.concatenate([one(ref, slot) for slot in range(3) for ref in refs], 0)

    def masks(self, mask_ref, row_mask_ref, slot):
        return self.tiles(
            lambda rows, o: row_mask_ref[rows][:, None, :] * mask_ref[pl.ds(o, self.size)][None], self.length, slot
        )

    def column_masks(self, mask_ref, slots):
        return jnp.concatenate([mask_ref[pl.ds(o, self.size)] for t in slots for o in self.slots()[t]], 0)


def keep(place, step, ref, w_ref):
    part = ref.shape[2]
    at = pl.multiple_of((place.chan ^ step) * part, part)
    w_ref[:, :, pl.ds(at, part), :] = ref[...] * jnp.bfloat16(0.5)


def early_kernel(counts, *refs):
    present_ref, ig_ref, ib_ref = refs[:3]
    sources = refs[3:9]
    gate_ref, x_ref, w_ref, mask_ref, row_mask_ref, gw_ref, fold_ref, shift_ref, normed_ref = refs[9:18]
    raw, sems = refs[18:24], refs[24]
    copies = [pltpu.make_async_copy(a, b, sems.at[i]) for i, (a, b) in enumerate(zip(sources, raw))]
    for copy in copies:
        copy.start()
    length, h = mask_ref.shape
    place = Place(counts, length, x_ref.shape[2])
    half = jnp.bfloat16(0.5)
    across = present_ref[...].astype(jnp.float32)
    square = (length, length)
    diagonal = lax.broadcasted_iota(jnp.int32, square, 0) == lax.broadcasted_iota(jnp.int32, square, 1)
    mask_ref[...] = mm(jnp.where(diagonal, across, 0.0).astype(jnp.bfloat16), jnp.ones((length, h), jnp.bfloat16))
    for i, where in enumerate(place.early + place.late):
        row_mask_ref[i * place.size:(i + 1) * place.size] = mask_ref[pl.ds(place.at(*where), place.size)]
    for copy in copies:
        copy.wait()
    pair_ref, projections_ref, gate_weight_ref, ow_ref, og_ref, ob_ref = raw
    gw_ref[...] = gate_weight_ref[...] * half
    keep(place, 0, projections_ref, w_ref)
    normed_ref[...] = place.enter([pair_ref[...]], ig_ref, ib_ref, gw_ref, gate_ref, x_ref)
    for layer in range(2):
        out = ow_ref[layer] * half
        folded = exact(place.centring.astype(jnp.float32) * og_ref[layer:layer + 1], out)
        high = folded.astype(jnp.bfloat16)
        fold_ref[layer, :h, :h] = place.centring
        fold_ref[layer, :h, h:] = high
        fold_ref[layer, h:, :h] = jnp.zeros((h, h), jnp.bfloat16)
        fold_ref[layer, h:, h:] = (folded - high.astype(jnp.float32)).astype(jnp.bfloat16)
        shift_ref[layer] = exact(jnp.broadcast_to(ob_ref[layer:layer + 1], (8, h)), out)


def arrived_kernel(counts, *refs):
    n = counts[0]
    blocks = refs[:n]
    ig_ref, ib_ref, gw_ref, own_ref, gate_ref, x_ref, normed_ref = refs[n:]
    place = Place(counts, x_ref.shape[1], x_ref.shape[2])
    normed_ref[0] = own_ref[...]
    normed = place.enter([b[...] for b in blocks], ig_ref, ib_ref, gw_ref, gate_ref, x_ref)
    normed_ref[1:] = normed.reshape(n, place.area, place.c)


def first_kernel(counts, ahead, *refs):
    n = counts[1] - 1
    weights = refs[:n]
    normed_ref, mask_ref, row_mask_ref, _, left_ref, turned_ref, tri_ref, w_ref = refs[n:]
    place = Place(counts, mask_ref.shape[0], normed_ref.shape[2])
    for i, ref in enumerate(weights):
        keep(place, i + 1, ref, w_ref)
    rows = left_ref.shape[0]
    mask = mask_ref[...]
    size = place.size
    wanted = jnp.concatenate([normed_ref[0], *[normed_ref[rs] for rs in place.chips()]], 0)
    right = place.edges(wanted, w_ref, 2, place.column_masks(mask_ref, (0, 1))[:, None, :] * mask[None])
    turned_ref[0] = place.turned(right[:size])
    turned_ref[1] = place.turned(right[size:])
    every = normed_ref[...].reshape(-1, place.c)
    left_ref[...] = place.edges(every, w_ref, 0, row_mask_ref[:rows][:, None, :])
    for i in range(0, ahead, size):
        place.triangle(
            left_ref, i, size, {0: turned_ref.at[0], 1: turned_ref.at[1]}, {0: (tri_ref, 0), 1: (tri_ref, ahead // 2)}
        )


def last_kernel(counts, ahead, *refs):
    n = counts[0] - 1
    blocks = refs[:n]
    (ig_ref, ib_ref, left_ref, turned_ref, tri_ref, gate0_ref, x0_ref, gate1_ref, x1_ref, normed_ref, w_ref, mask_ref,
     row_mask_ref, gw_ref, fold_ref, shift_ref, out_ref,
     gate2_ref, x2_ref, others_ref, late_ref, turned2_ref, tri0_ref, tri1_ref, tri2_ref, l1_ref, r1_ref) = refs[n:]
    length, h = mask_ref.shape
    c = x0_ref.shape[2]
    place = Place(counts, length, c)
    size, chip, quarter = place.size, place.chip, place.quarter
    rows = left_ref.shape[0]
    mask = mask_ref[...]
    early_turned = {0: turned_ref.at[0], 1: turned_ref.at[1]}
    for i in range(ahead, rows, size):
        place.triangle(left_ref, i, size, early_turned, {0: (tri0_ref, -ahead // 2), 1: (tri1_ref, -ahead)})
    normed = place.enter([b[...] for b in blocks], ig_ref, ib_ref, gw_ref, gate2_ref, x2_ref)
    others_ref[0] = normed_ref[counts[0]]
    others_ref[1:] = normed.reshape(n, place.area, c)
    wanted = jnp.concatenate([others_ref[rs] for rs in place.chips()], 0)
    turned2_ref[...] = place.turned(
        place.edges(wanted, w_ref, 2, place.column_masks(mask_ref, (2,))[:, None, :] * mask[None])
    )
    late_ref[...] = place.edges(normed, w_ref, 0, row_mask_ref[rows:][:, None, :])
    for i in range(0, rows, 2 * size):
        place.triangle(left_ref, i, min(2 * size, rows - i), {2: turned2_ref}, {2: (tri2_ref, 0)})
    late = late_ref.shape[0]
    for i in range(0, late, size):
        place.triangle(
            late_ref, i, size, {**early_turned, 2: turned2_ref},
            {0: (tri0_ref, (rows - ahead) // 2), 1: (tri1_ref, rows - ahead), 2: (tri2_ref, rows)},
        )

    def finish(tri, half_gate, residual, layer):
        both = tri.astype(jnp.bfloat16)
        both = mm(jnp.concatenate([both, both], 1), fold_ref[layer])
        centred = both[:, :h]
        spread = jnp.mean(centred * centred, axis=1, keepdims=True)
        update = both[:, h:] * lax.rsqrt(spread + epsilon) + shift_ref[layer, 0:1]
        return (residual + update * half_gate).astype(jnp.bfloat16)

    half_gate = place.columns((gate0_ref, gate1_ref, gate2_ref))
    residual = place.columns((x0_ref, x1_ref, x2_ref))
    tri = jnp.concatenate([tri_ref[:ahead // 2], tri0_ref[...], tri_ref[ahead // 2:], tri1_ref[...], tri2_ref[...]], 0)
    z = finish(tri.reshape(residual.shape[0], h), half_gate, residual, 0)
    area = length * size

    normed = place.norm(z, ig_ref, ib_ref, 1)
    starts = [area + t * length * chip for t in range(2)]
    mine = jnp.concatenate([z[a:a + size * chip] for a in starts], 0).astype(jnp.float32)
    mine_normed = jnp.concatenate([normed[a:a + size * chip] for a in starts], 0)
    p = mmt(normed[:area], w_ref[1, 0:2].reshape(2 * h, c))
    l1_ref[...] = gated(p[:, :h], p[:, h:] * place.masks(mask_ref, row_mask_ref, 0))
    p = mmt(normed[area:], w_ref[1, 2:4].reshape(2 * h, c))
    area = length * chip
    for t in (1, 2):
        at = slice((t - 1) * area, t * area)
        columns = place.column_masks(mask_ref, (t,))[None]
        shape = (length, chip, h)
        r1_ref[t - 1] = gated(p[at, :h].reshape(shape), p[at, h:].reshape(shape) * columns)
    half_gate = 1.0 + jnp.tanh(mm(mine_normed, gw_ref[1]))

    acc = [jnp.zeros((chip, h), jnp.float32) for _ in range(2 * size)]
    for k in range(length):
        rs = [r1_ref[t, k] for t in range(2)]
        ls = [l1_ref[k * size + i:k * size + i + 1, :] for i in range(size)]
        acc = [acc[t * size + i] + ls[i] * rs[t] for t in range(2) for i in range(size)]
    z = finish(jnp.concatenate(acc, 0), half_gate, mine, 1).astype(jnp.float32).reshape(2, size, chip, c)
    even = jnp.where(place.sub == 0, z[0], z[1])
    odd = jnp.where(place.sub == 0, z[1], z[0])
    parts = [v[:, i * size:(i + 1) * size] for i in range(quarter // chip) for v in (even, odd)]
    out_ref[...] = jnp.concatenate(parts, 1).astype(jnp.bfloat16)


def in_vmem(value):
    return pltpu.with_memory_space_constraint(value, pltpu.VMEM)


def in_hbm(value):
    return pltpu.with_memory_space_constraint(value, pltpu.HBM)


VMEM = pl.BlockSpec(memory_space=pltpu.VMEM)
HBM = pl.BlockSpec(memory_space=pltpu.HBM)

AHEAD = 12


def gathered(
    pair, residue_mask, in_gain, in_bias, projections, gate_weight, out_gain, out_bias, out_weight
):
    rows_count, chan_count, sub_count = (lax.axis_size(a) for a in ("rows", "chan", "sub"))
    size, length, c = pair.shape
    h = out_weight.shape[1]
    chip, area = size * sub_count, size * length
    counts = (rows_count, chan_count, sub_count, size)
    turned = jnp.swapaxes(projections, 2, 3)
    hops = tuple(range(1, rows_count))
    far, near = {}, {}
    for rs in hops:
        far[rs] = swap(pair, "rows", rs)
    near[0] = swap(pair, "sub", 1)
    weights = [swap(turned, "chan", i) for i in range(1, chan_count)]
    for rs in hops:
        near[rs] = swap(far[rs], "sub", 1)

    def f32(*shape):
        return pltpu.VMEM(shape, jnp.float32)

    def bf16(*shape):
        return pltpu.VMEM(shape, jnp.bfloat16)

    def call(kernel, near, far, out_shape, scratch=(), aliases={}, rows=0, mib=8):
        return pl.pallas_call(
            kernel,
            out_shape=out_shape,
            in_specs=[VMEM] * len(near) + [HBM] * len(far),
            out_specs=jax.tree.map(lambda _: VMEM, out_shape),
            scratch_shapes=[
                *scratch,
                *[pltpu.VMEM(o.shape, o.dtype) for o in far],
                *([pltpu.SemaphoreType.DMA((len(far),))] if far else []),
            ],
            input_output_aliases=aliases,
            compiler_params=pltpu.CompilerParams(vmem_limit_bytes=mib << 20),
            cost_estimate=pl.CostEstimate(flops=rows * c * c * 16, bytes_accessed=0, transcendentals=0),
        )(*[in_vmem(o) for o in near], *[in_hbm(o) for o in far])

    gate0, x0, w, mask, row_mask, gw, fold, shift, own = call(
        functools.partial(early_kernel, counts),
        [residue_mask[None], in_gain, in_bias],
        [pair, turned, gate_weight, out_weight, out_gain, out_bias],
        [
            f32(size, length, c),
            f32(size, length, c),
            bf16(2, 4, h, c),
            f32(length, h),
            f32(length, h),
            bf16(2, c, c),
            bf16(2, 2 * h, h + c),
            f32(2, 8, c),
            bf16(area, c),
        ],
        rows=length * length,
    )
    gate1, x1, normed = call(
        functools.partial(arrived_kernel, counts),
        [*[far[rs] for rs in hops], near[0], in_gain, in_bias, gw, own],
        [],
        [
            f32(rows_count * size, length, c),
            f32(rows_count * size, length, c),
            bf16(rows_count + 1, area, c),
        ],
        rows=length * length,
    )
    early = (rows_count + 1) * size
    late = length - early
    operands = [*weights, normed, mask, row_mask, w]
    left, right, tri, w = call(
        functools.partial(first_kernel, counts, AHEAD),
        operands,
        [],
        [f32(early, length, h), f32(2, length, chip, h), f32(AHEAD // 2 + AHEAD, chip, h), bf16(2, 4, h, c)],
        aliases={len(operands) - 1: 3},
        rows=length * length,
    )
    operands = [
        *[near[rs] for rs in hops], in_gain, in_bias, left, right, tri, gate0, x0, gate1, x1, normed, w, mask, row_mask,
        gw, fold, shift,
    ]
    return call(
        functools.partial(last_kernel, counts, AHEAD),
        operands,
        [],
        jax.ShapeDtypeStruct((size, length // chan_count, c), jnp.bfloat16),
        scratch=[
            f32(late, length, c),
            f32(late, length, c),
            bf16(rows_count, area, c),
            f32(late, length, h),
            f32(length, chip, h),
            f32((length - AHEAD) // 2, chip, h),
            f32(length - AHEAD, chip, h),
            f32(length, chip, h),
            f32(length * size, h),
            f32(2, length, chip, h),
        ],
        rows=1,
        mib=16,
    )


def solution(mesh):
    def body(pair, *rest):
        size, length, c = pair.shape
        small = 2 * length * length * c <= GATHER_LIMIT
        fits = (
            mesh.shape["sub"] == 2
            and mesh.shape["rows"] & (mesh.shape["rows"] - 1) == 0
            and size * 2 == 8
            and length == 16 * mesh.shape["chan"]
        )
        if not (small and fits):
            return shards(pair, *rest)
        return gathered(pair, *rest)

    placed = (
        P(("crops", "rows", "sub"), None, None),
        P("crops"),
        P(),
        P(),
        P(None, None, None, "chan"),
        P(),
        P(),
        P(),
        P(),
    )
    step = jax.shard_map(
        body,
        mesh=mesh,
        in_specs=placed,
        out_specs=P(("crops", "rows", "sub"), "chan", None),
        check_vma=False,
    )
    if 8 * mesh.shape["rows"] != 16 * mesh.shape["chan"]:
        return step
    return step
```
